512 devices in a mesh: row: 32 (over x, y, core), col: 16 (over z).
Axes of the slice: x: 4, y: 4, z: 16, core: 2. Of those that a mesh axis runs over, the one named last changes fastest.
Arguments:
- vis: float32 [2, 4194304], P(None, ('row', 'col')), may hold values from -6 to 6
- vis_pos: int32 [2, 4194304], P(None, ('row', 'col')), may hold values from 0 to 199
- vis_w: int32 [4194304], P(('row', 'col')), may hold values from 0 to 1023
- subgrid_tile: int32 [16384, 1], P(('row', 'col')), may hold values from 0 to 15; in each aligned block of 32 rows (0 to 31, 32 to 63, ...) at most 4 rows name the same one
- subgrid_group: int32 [16384, 1], P(('row', 'col')), may hold values from 0 to 14; in each aligned block of 32 rows (0 to 31, 32 to 63, ...) at most 4 rows name the same one
- subgrid_col: int32 [16384], P(('row', 'col')), may hold values from 0 to 480
- grid_kernel: float32 [8, 8], replicated, may hold values from 0.1 to 1
- scale_kernels: float32 [2, 33], replicated, may hold values from -1 to 1
Outputs:
- scale_images: float32 [2, 8192, 8192], P(None, ('row', 'col'))
The draws below stay inside these ranges and needn't reach their ends.
Inputs may be any that keep to these rules, and one draw needn't show every extreme that they name: `vis_pos`: row 0 counts along grid rows, row 1 along grid columns, in steps of 1/8 cell from the corner of the visibility's subgrid. `subgrid_tile`: among the subgrids of one device (aligned blocks of 32), at most 4 name the same column tile; in some blocks one tile is named exactly that often. `subgrid_group`: among the subgrids of one device (aligned blocks of 32), at most 4 name the same row group; in some blocks one group is named exactly that often.
All inputs are finite; a program needn't handle non-finite values.
Results may differ from the reference program's by a relative error of at most 0.0003.
Values sent between devices are 32-bit elements; how exact they have to be, the bound alone decides.
A program may use at most 64 MiB of HBM per device.

```python
import math
import jax
import jax.numpy as jnp
import numpy as np
from jax import lax

G = 8192
SUB = 32
SUP = 8
OVER = 8
VPS = 256
WSTEPS = 1024
KW = 33
NSCALE = 2
SUBS_DEV = 32
SUBS = 16384
VIS = 4194304
TC = 512
NGRP = 15
CAPT = 4
MOSTG = 4
N_ROW = 32
N_COL = 16


def touch_ends(drawn, own_key, smallest, largest):
    place = [jax.random.randint(jax.random.fold_in(own_key, axis), (), 0, length) for axis, length in enumerate(drawn.shape)]
    main_axis = drawn.shape.index(max(drawn.shape))
    neighbour = place[:main_axis] + [(place[main_axis] + 1) % drawn.shape[main_axis]] + place[main_axis + 1:]
    return drawn.at[tuple(place)].set(smallest).at[tuple(neighbour)].set(largest)


def shard_levels(stream_key, shape, pieces, smallest, largest):
    def one(axis_at, blocks):
        heights = jax.random.uniform(jax.random.fold_in(jax.random.fold_in(stream_key, 6), axis_at), (blocks,), jnp.float32, smallest / len(pieces), largest / len(pieces))
        return jnp.repeat(jnp.exp(heights), shape[axis_at] // blocks).reshape((-1,) + (1,) * (len(shape) - axis_at - 1))

    level = one(*pieces[0])
    for cut in pieces[1:]:
        level = level * one(*cut)
    return level


def deal_out(stream_key, own, number, rows, amount, top, most, lean):
    ranking = jax.random.permutation(stream_key, amount)
    packed, usual = portions_of(amount, rows * top, most, lean, True), portions_of(amount, rows * top, most, lean, False)
    places = jnp.arange(amount)

    def named(lengths, offset_by):
        used = int((lengths > 0).sum())
        fixed = max(1, used // 4)
        passed = fixed + (places - fixed + offset_by * (used - fixed)) % max(1, amount - fixed)
        return jnp.zeros((amount,), jnp.int32).at[ranking[jnp.where(places < fixed, places, passed)]].set(jnp.asarray(lengths, jnp.int32))

    lengths = jnp.where(number % 4 == 0, named(packed, number // 4), named(usual, number - number // 4 - 1))
    mixed = jax.random.permutation(jax.random.fold_in(own, 3), amount)
    donor, sink = mixed[0:amount // 2 * 2:2], mixed[1:amount // 2 * 2:2]
    margin = jnp.minimum(lengths[donor] - 1, most - lengths[sink]) // 2
    margin = jnp.where((donor == ranking[0]) | (sink == ranking[0]) | (lengths[sink] == 0), 0, jnp.maximum(margin, 0))
    passed = jax.random.randint(jax.random.fold_in(own, 4), (amount // 2,), 0, 1 << 20) % (margin + 1)
    lengths = lengths.at[donor].add(-passed).at[sink].add(passed)
    items = jnp.searchsorted(jnp.cumsum(lengths), jnp.arange(rows * top), side="right").astype(jnp.int32)
    listing = items.reshape(top, rows).T
    listing = listing[jax.random.permutation(jax.random.fold_in(own, 1), rows)]
    offset_by = jax.random.randint(jax.random.fold_in(own, 2), (rows, 1), 0, top)
    return jnp.take_along_axis(listing, (jnp.arange(top)[None, :] + offset_by) % top, axis=1)


def portions_of(amount, total, bound, slope, full):
    weights = [(1 << 20) // math.isqrt(rank ** slope) + 1 for rank in range(1, amount + 1)]
    largest = bound if full else min(bound, max(-(-total // amount), total * weights[0] // sum(weights)))
    least = 1 if total - largest >= amount - 1 else 0
    counts, rest = [largest] + [least] * (amount - 1), total - largest - least * (amount - 1)
    while rest > 0:
        candidates = [i for i in range(1, amount) if counts[i] < largest] or [i for i in range(1, amount) if counts[i] < bound]
        mass, left = sum([weights[i] for i in candidates]), rest
        for i in candidates:
            more = min(bound - counts[i], max(1, left * weights[i] // mass), rest)
            counts[i] = counts[i] + more
            rest = rest - more
    return np.array(counts)


def gaussian(key, shape, scale, most, split=(), kind=jnp.bfloat16):
    values = jax.random.normal(key, shape, jnp.float32) * scale
    if len(split) > 0:
        values = shard_levels(key, shape, split, -0.22, 0.18) * values
    return jnp.clip(values, min=-most, max=most).astype(kind)


def setup_inputs(seed: int = 0) -> dict:
    keys = jax.random.split(jax.random.key(seed), 9)
    vis = gaussian(keys[0], (2, VIS), 1.0, 6.0, ((1, 512),), jnp.float32)
    vis_pos = touch_ends(jax.random.randint(keys[1], (2, VIS), 0, (SUB - SUP + 1) * OVER), jax.random.fold_in(keys[1], 1), 0, ((SUB - SUP + 1) * OVER) - 1).astype(jnp.int32)
    vis_w = touch_ends(jax.random.randint(keys[2], (VIS,), 0, WSTEPS), jax.random.fold_in(keys[2], 1), 0, WSTEPS - 1).astype(jnp.int32)
    subgrid_tile_keys = jax.random.split(jax.random.fold_in(keys[3], 1), SUBS // SUBS_DEV)
    subgrid_tile_turns = jax.random.permutation(jax.random.fold_in(keys[3], 3), SUBS // SUBS_DEV)
    subgrid_tile = jax.vmap(lambda own, number: deal_out(jax.random.fold_in(keys[3], 2), own, number, SUBS_DEV, N_COL, 1, CAPT, 2))(subgrid_tile_keys, subgrid_tile_turns).reshape((SUBS, 1))
    subgrid_group_keys = jax.random.split(jax.random.fold_in(keys[4], 1), SUBS // SUBS_DEV)
    subgrid_group_turns = jax.random.permutation(jax.random.fold_in(keys[4], 3), SUBS // SUBS_DEV)
    subgrid_group = jax.vmap(lambda own, number: deal_out(jax.random.fold_in(keys[4], 2), own, number, SUBS_DEV, NGRP, 1, MOSTG, 1))(subgrid_group_keys, subgrid_group_turns).reshape((SUBS, 1))
    subgrid_col = touch_ends(jax.random.randint(keys[5], (SUBS,), 0, TC - SUB + 1), jax.random.fold_in(keys[5], 1), 0, TC - SUB).astype(jnp.int32)
    grid_kernel = jnp.clip(jnp.exp(jax.random.uniform(keys[6], (OVER, SUP), jnp.float32, math.log(0.1), math.log(1.0))), 0.1, 1.0)
    scale_kernels = gaussian(keys[7], (NSCALE, KW), KW ** -0.5, 1.0, (), jnp.float32)
    return {"vis": vis, "vis_pos": vis_pos, "vis_w": vis_w, "subgrid_tile": subgrid_tile, "subgrid_group": subgrid_group, "subgrid_col": subgrid_col, "grid_kernel": grid_kernel, "scale_kernels": scale_kernels}


HIGHEST = lax.Precision.HIGHEST


def kernel_taps(positions, grid_kernel):
    cell_index = positions // OVER
    fraction = positions % OVER
    onehot = (fraction[:, None] == jnp.arange(OVER, dtype=jnp.int32)[None, :]).astype(grid_kernel.dtype)
    values = jnp.dot(onehot, grid_kernel, precision=HIGHEST)
    offset = jnp.arange(SUB, dtype=jnp.int32)[None, :] - cell_index[:, None]
    result = jnp.zeros(offset.shape, grid_kernel.dtype)
    for tap_index in range(SUP):
        result = result + jnp.where(offset == tap_index, values[:, tap_index:tap_index + 1], 0.0)
    return result


def make_subgrids(vis_block, pos_block, phase_steps, grid_kernel, number):
    along_rows = kernel_taps(pos_block[0], grid_kernel).reshape(number, VPS, SUB)
    along_cols = kernel_taps(pos_block[1], grid_kernel).reshape(number, VPS, SUB)
    angles = phase_steps.astype(grid_kernel.dtype) * (2.0 * math.pi / WSTEPS)
    cosine = jnp.cos(angles)
    sine_part = jnp.sin(angles)
    rotated_real = vis_block[0] * cosine + vis_block[1] * sine_part
    rotated_imag = vis_block[1] * cosine - vis_block[0] * sine_part
    weighted_real = along_rows * rotated_real.reshape(number, VPS, 1)
    weighted_imag = along_rows * rotated_imag.reshape(number, VPS, 1)
    sub_real = jnp.einsum('sja,sjb->sab', weighted_real, along_cols, precision=HIGHEST)
    sub_imag = jnp.einsum('sja,sjb->sab', weighted_imag, along_cols, precision=HIGHEST)
    return sub_real, sub_imag


def reference(vis, vis_pos, vis_w, subgrid_tile, subgrid_group, subgrid_col, grid_kernel, scale_kernels):
    band_rows = G // N_ROW
    tile_width = G // N_COL
    group_rows = band_rows // N_COL
    per_device = SUBS_DEV * VPS
    cell_offsets = (jnp.arange(SUB, dtype=jnp.int32)[:, None] * G + jnp.arange(SUB, dtype=jnp.int32)[None, :]).reshape(-1)

    def add_device(carry, device):
        grid_real, grid_imag = carry
        start = device * per_device
        vis_block = lax.dynamic_slice_in_dim(vis, start, per_device, 1)
        pos_block = lax.dynamic_slice_in_dim(vis_pos, start, per_device, 1)
        phase_block = lax.dynamic_slice_in_dim(vis_w, start, per_device, 0)
        first_sub = device * SUBS_DEV
        tile_index = lax.dynamic_slice_in_dim(subgrid_tile[:, 0], first_sub, SUBS_DEV, 0)
        groups = lax.dynamic_slice_in_dim(subgrid_group[:, 0], first_sub, SUBS_DEV, 0)
        columns = lax.dynamic_slice_in_dim(subgrid_col, first_sub, SUBS_DEV, 0)
        band_index = device // N_COL
        corner_row = band_index * band_rows + groups * group_rows
        corner_col = tile_index * tile_width + columns
        sub_real, sub_imag = make_subgrids(vis_block, pos_block, phase_block, grid_kernel, SUBS_DEV)
        targets = ((corner_row * G + corner_col)[:, None] + cell_offsets[None, :]).reshape(-1)
        grid_real = grid_real.at[targets].add(sub_real.reshape(-1))
        grid_imag = grid_imag.at[targets].add(sub_imag.reshape(-1))
        return (grid_real, grid_imag), None

    zeros = jnp.zeros((G * G,), vis.dtype)
    (grid_real, grid_imag), unused = lax.scan(add_device, (zeros, zeros), jnp.arange(N_ROW * N_COL, dtype=jnp.int32))
    grid = lax.complex(grid_real, grid_imag).reshape(G, G)
    image = jnp.real(jnp.fft.ifft2(grid)) * G
    image = image.T
    halo_width = (KW - 1) // 2
    vertical = lax.conv_general_dilated(image[None, None], scale_kernels[:, None, None, :], (1, 1), ((0, 0), (halo_width, halo_width)), precision=HIGHEST)
    smoothed = lax.conv_general_dilated(vertical, scale_kernels[:, None, :, None], (1, 1), ((halo_width, halo_width), (0, 0)), feature_group_count=NSCALE, precision=HIGHEST)
    return smoothed[0]
```

```python
import functools
import math

import jax
import jax.numpy as jnp
import ml_dtypes
import numpy as np
from jax import lax
from jax.experimental import pallas as pl
from jax.experimental.pallas import tpu as pltpu
from jax.sharding import PartitionSpec as P

G = 8192
SUB = 32
SUP = 8
OVER = 8
VPS = 256
WSTEPS = 1024
KW = 33
NSCALE = 2
NR = 32
NC = 16
SD = 32
HALO = 16
MSG = SD + 8

BF = jnp.bfloat16
F32 = jnp.float32
MESH = pl.DeviceIdType.MESH
NN = (((1,), (0,)), ((), ()))
NT = (((1,), (1,)), ((), ()))
VM = pl.BlockSpec(memory_space=pltpu.VMEM)
SM = pl.BlockSpec(memory_space=pltpu.SMEM)


def two_parts(x):
    high = x.astype(BF)
    return high, (x - high.astype(F32)).astype(BF)


def dot(a, b, dims=NN):
    return lax.dot_general(a, b, dims, preferred_element_type=F32)


def np_parts(x):
    x = np.asarray(x, np.float64)
    high = x.astype(np.float32).astype(ml_dtypes.bfloat16)
    low = (x - high.astype(np.float64)).astype(np.float32).astype(ml_dtypes.bfloat16)
    return high, low


def angle_tables(a, b, period):
    turn = 2.0 * math.pi * ((np.asarray(a, np.int64) * np.asarray(b, np.int64)) % period) / period
    return np.cos(turn), np.sin(turn)


def row_tables():
    q0 = np.arange(64)
    cos, sin = angle_tables(q0[:, None], q0[None, :], 64)
    first_h, first_l = np_parts(np.concatenate([cos, sin], 0))
    first = np.concatenate([first_h, first_l, first_h], 1)
    cos, sin = angle_tables(q0[:, None], np.arange(128)[None, :], G)
    twiddle = np.stack([cos, sin]).astype(np.float32)
    high = (4 * np.arange(NR)[None, :] + np.arange(4)[:, None]).reshape(-1)
    cos, sin = angle_tables(high[:, None], np.arange(128)[None, :], 128)
    second = np.concatenate(
        [np.concatenate([cos, -sin], 1), np.concatenate([sin, cos], 1)], 0
    )
    return (first, twiddle, *np_parts(second))


def column_tables():
    p0 = np.arange(NR)
    cos, sin = angle_tables(p0[:, None], p0[None, :], NR)
    full = np.concatenate([np.concatenate([cos, -sin], 1), np.concatenate([sin, cos], 1)], 0)
    first_h, first_l = np_parts(full)
    first = np.concatenate([first_h, first_l, first_h], 1)
    r = np.arange(256) // 16
    cos, sin = angle_tables(p0[:, None], r[None, :], 512)
    turn_one = np.stack([cos, sin]).astype(np.float32)
    d = np.arange(16)
    cos, sin = angle_tables(d[:, None], d[None, :], 16)
    eye = np.eye(16)
    cos, sin = np.kron(cos, eye), np.kron(sin, eye)
    second = np.concatenate([np.concatenate([cos, -sin], 1), np.concatenate([sin, cos], 1)], 0)
    c = np.repeat(d, NR)
    cos, sin = angle_tables(c[None, :], np.tile(p0, 16)[None, :] + NR * d[:, None], G)
    turn_two = np.stack([cos, sin]).astype(np.float32)
    cos, sin = angle_tables(d[:, None], d[None, :], 16)
    eye = np.eye(NR)
    third = np.concatenate([np.kron(cos, eye), -np.kron(sin, eye)], 0) / G
    return (first, turn_one, *np_parts(second), turn_two, *np_parts(third))


def gridding_kernel(l0_ref, vis_ref, pos_ref, w_ref, taps_ref, meta_ref, out_ref):
    for c in range(NC):
        out_ref[pl.ds(c * MSG + SD, 8), :] = meta_ref[...]
    columns = [jnp.broadcast_to(taps_ref[:, t : t + 1], (SUP, VPS)) for t in range(OVER)]
    cell_axis = lax.broadcasted_iota(jnp.int32, (SUB, VPS), 0)

    def weights(pos):
        step = jnp.broadcast_to(pos & (OVER - 1), (SUP, VPS))
        rows = columns[0]
        for t in range(1, OVER):
            rows = jnp.where(step == t, columns[t], rows)
        return rows

    def spread(rows, distance):
        out = jnp.zeros((SUB, VPS), F32)
        for t in range(SUP):
            out = jnp.where(distance == t, jnp.broadcast_to(rows[t : t + 1, :], (SUB, VPS)), out)
        return out

    def one(s, carry):
        here = pl.ds(pl.multiple_of(s * VPS, VPS), VPS)
        pos_u, pos_v = pos_ref[0:1, here], pos_ref[1:2, here]
        angle = w_ref[0:1, here].astype(F32) * (2.0 * math.pi / WSTEPS)
        cosine, sine = jnp.cos(angle), jnp.sin(angle)
        real, imag = vis_ref[0:1, here], vis_ref[1:2, here]
        turned_real = real * cosine + imag * sine
        turned_imag = imag * cosine - real * sine
        along_u = spread(weights(pos_u), cell_axis - lax.shift_right_logical(pos_u, 3))
        start = l0_ref[s] & (SUB - 1)
        along_v = spread(
            weights(pos_v),
            (cell_axis - lax.shift_right_logical(pos_v, 3) - start) & (SUB - 1),
        )
        left_h, left_l = two_parts(
            jnp.concatenate([along_u * turned_real, along_u * turned_imag], axis=0)
        )
        right_h, right_l = two_parts(along_v)
        block = dot(left_h, right_h, NT) + dot(left_l, right_h, NT) + dot(left_h, right_l, NT)
        block = jnp.concatenate([block[i * 16 : (i + 1) * 16] for i in range(4)], axis=1)
        out_ref[pl.ds(s, NC, stride=MSG), :] = block
        return carry

    lax.fori_loop(0, SD, one, 0, unroll=2)


def spread_kernel(send_ref, recv_ref, send_sem, recv_sem, own_sem):
    row, col = lax.axis_index("row"), lax.axis_index("col")
    barrier = pltpu.get_barrier_semaphore()
    for d in range(1, NC):
        pl.semaphore_signal(
            barrier, inc=1, device_id=(row, lax.rem(col + d, NC)), device_id_type=MESH
        )
    own = pltpu.make_async_copy(send_ref.at[col], recv_ref.at[col], own_sem)
    own.start()
    pl.semaphore_wait(barrier, NC - 1)

    def copy(d):
        to = lax.rem(col + d, NC)
        return pltpu.make_async_remote_copy(
            src_ref=send_ref.at[to],
            dst_ref=recv_ref.at[col],
            send_sem=send_sem.at[d],
            recv_sem=recv_sem.at[d],
            device_id=(row, to),
            device_id_type=MESH,
        )

    order = [8] + [d for i in range(7, 0, -1) for d in (i, NC - i)]
    for d in order:
        copy(d).start()
    own.wait()
    for d in order:
        copy(d).wait()


def rows_kernel(recv_ref, first_ref, turn_ref, second_h, second_l, out_ref, u_h, u_l, a_h, a_l):
    lane = lax.broadcasted_iota(jnp.int32, (SD, 128), 1)
    sub = lax.broadcasted_iota(jnp.int32, (SD, 128), 0)
    segment = lax.shift_right_logical(lane, 5)

    def unpack(z, carry):
        data = recv_ref[z, 0:SD, :]
        corner = recv_ref[z, SD : SD + 1, :]
        mine = lane == sub + SD * (z & 3)
        l0 = jnp.sum(
            jnp.where(mine, jnp.broadcast_to(corner, (SD, 128)), 0.0), axis=1, keepdims=True
        )
        distance = lane - (l0.astype(jnp.int32) & 127)
        in_a = (distance >= 0) & (distance < SUB)
        in_b = distance < SUB - 128
        rolled = [data] + [pltpu.roll(data, SUB * k, 1) for k in range(1, 4)]
        wide = []
        for i in range(4):
            v = rolled[(0 - i) % 4]
            for p in range(1, 4):
                v = jnp.where(segment == p, rolled[(p - i) % 4], v)
            wide.append(v)
        for hi in range(2):
            for ab, inside in enumerate((in_a, in_b)):
                v = jnp.concatenate(
                    [jnp.where(inside, wide[hi], 0.0), jnp.where(inside, wide[2 + hi], 0.0)],
                    axis=1,
                )
                high, low = two_parts(v)
                at = pl.ds(pl.multiple_of((hi * 2 + ab) * 512 + z * SD, SD), SD)
                u_h[at, :] = high
                u_l[at, :] = low
        return carry

    lax.fori_loop(0, NC, unpack, 0, unroll=2)

    index = []
    for group in range(4):
        corner = sum(recv_ref[group * 4 + i, SD : SD + 1, :] for i in range(4))
        start = sum(recv_ref[group * 4 + i, SD + 1 : SD + 2, :] for i in range(4))
        index.append(
            start.astype(jnp.int32) * 64
            + lax.shift_right_logical(corner.astype(jnp.int32), 7)
        )
    pairs = [jnp.concatenate(index[0:2], axis=1), jnp.concatenate(index[2:4], axis=1)]

    def four_rows(block, carry):
        place = lax.broadcasted_iota(jnp.int32, (256, 256), 0) + block * 256
        total = jnp.zeros((256, 256), F32)
        for hi in range(2):
            for ab in range(2):
                for half in range(2):
                    chunk = (hi * 2 + ab) * 2 + half
                    pick = (place == pairs[half] + (hi * 64 + ab)).astype(F32).astype(BF)
                    at = slice(chunk * 256, (chunk + 1) * 256)
                    total = total + dot(pick, u_h[at, :]) + dot(pick, u_l[at, :])
        for k in range(4):
            high, low = two_parts(total[k * 64 : (k + 1) * 64])
            both = dot(first_ref[...], jnp.concatenate([high, high, low], axis=0))
            real = both[:64, :128] - both[64:, 128:]
            imag = both[64:, :128] + both[:64, 128:]
            cos, sin = turn_ref[0], turn_ref[1]
            high, low = two_parts(
                jnp.concatenate([real * cos - imag * sin, real * sin + imag * cos], axis=1)
            )
            for cl in range(4):
                at = pl.ds(pl.multiple_of(cl * 256 + (block * 4 + k) * 16, 16), 16)
                a_h[at, :] = high[cl * 16 : (cl + 1) * 16]
                a_l[at, :] = low[cl * 16 : (cl + 1) * 16]
        return carry

    lax.fori_loop(0, 4, four_rows, 0)

    for cl in range(4):
        at = slice(cl * 256, (cl + 1) * 256)
        done = (
            dot(second_h[...], a_h[at, :], NT)
            + dot(second_l[...], a_h[at, :], NT)
            + dot(second_h[...], a_l[at, :], NT)
        )
        for ri in range(2):
            for ch in range(4):
                for half in range(2):
                    for part in range(4):
                        r0 = ri * 128 + ch * 32 + part * 8
                        out_ref[
                            pl.ds((4 * ch + cl) * 128 + part * 32 + ri * 2 + half, 8, stride=4), :
                        ] = done[r0 : r0 + 8, half * 128 : (half + 1) * 128]


def turn_kernel(send_ref, out_ref, mid_ref, send_a, recv_a, send_b, recv_b, own_a, own_b):
    row, col = lax.axis_index("row"), lax.axis_index("col")
    barrier = pltpu.get_barrier_semaphore()
    for d in range(1, NC):
        pl.semaphore_signal(
            barrier, inc=1, device_id=(row, lax.rem(col + d, NC)), device_id_type=MESH
        )
    for d in range(1, NR):
        pl.semaphore_signal(
            barrier, inc=1, device_id=(lax.rem(row + d, NR), col), device_id_type=MESH
        )
    own = pltpu.make_async_copy(send_ref.at[col], mid_ref.at[col], own_a)
    own.start()
    pl.semaphore_wait(barrier, NC - 1 + NR - 1)

    def first(d):
        to = lax.rem(col + d, NC)
        return pltpu.make_async_remote_copy(
            src_ref=send_ref.at[to],
            dst_ref=mid_ref.at[col],
            send_sem=send_a.at[d],
            recv_sem=recv_a.at[d],
            device_id=(row, to),
            device_id_type=MESH,
        )

    rings = [(1, 15, 2, 14), (3, 13, 4, 12), (5, 11, 6, 10), (7, 9, 8)]
    for ring in rings:
        for d in ring:
            first(d).start()

    def second(offset, e):
        source = lax.rem(col + NC - offset, NC)
        to = lax.rem(row + e, NR)
        return pltpu.make_async_remote_copy(
            src_ref=mid_ref.at[source, to],
            dst_ref=out_ref.at[source, row],
            send_sem=send_b.at[offset, e],
            recv_sem=recv_b.at[offset, e],
            device_id=(to, col),
            device_id_type=MESH,
        )

    def own_second(offset):
        source = lax.rem(col + NC - offset, NC)
        return pltpu.make_async_copy(
            mid_ref.at[source, row], out_ref.at[source, row], own_b.at[offset]
        )

    own.wait()
    for d in (0,) + sum(rings, ()):
        if d:
            first(d).wait()
        own_second(d).start()

        def send(e, carry, d=d):
            second(d, e).start()
            return carry

        lax.fori_loop(1, NR, send, 0)
    for d in range(NC):
        own_second(d).wait()

        def finish(e, carry, d=d):
            second(d, e).wait()
            return carry

        lax.fori_loop(1, NR, finish, 0)


def columns_kernel(
    in_ref, first_ref, turn_one, second_h, second_l, turn_two, third_h, third_l, out_ref,
    y_h, y_l, z_h, z_l, image
):
    def one(c, carry):
        def piece(i):
            return in_ref[pl.ds(c * 128 + i, NR, stride=4), :]

        value = jnp.concatenate(
            [
                jnp.concatenate([piece(0), piece(1)], axis=1),
                jnp.concatenate([piece(2), piece(3)], axis=1),
            ],
            axis=0,
        )
        high, low = two_parts(value)
        done = dot(first_ref[...], jnp.concatenate([high, high, low], axis=0))
        real, imag = done[:NR], done[NR:]
        cos, sin = turn_one[0], turn_one[1]
        high, low = two_parts(
            jnp.concatenate([real * cos - imag * sin, real * sin + imag * cos], axis=1)
        )
        at = pl.ds(pl.multiple_of(c * NR, NR), NR)
        y_h[at, :] = high
        y_l[at, :] = low
        return carry

    lax.fori_loop(0, NC, one, 0, unroll=2)

    def four_digits(block, carry):
        base = pl.multiple_of(block * 64, 64)
        parts = []
        for ri in range(2):
            at = pl.ds(ri * 256 + base, 64)
            parts.append(
                dot(second_h[at, :], y_h[...], NT)
                + dot(second_l[at, :], y_h[...], NT)
                + dot(second_h[at, :], y_l[...], NT)
            )
        for k in range(4):
            real, imag = parts[0][k * 16 : (k + 1) * 16], parts[1][k * 16 : (k + 1) * 16]
            cos = turn_two[0, pl.ds(block * 4 + k, 1), :]
            sin = turn_two[1, pl.ds(block * 4 + k, 1), :]
            high, low = two_parts(
                jnp.concatenate([real * cos - imag * sin, real * sin + imag * cos], axis=1)
            )
            at = pl.ds(base + k * 16, 16)
            z_h[at, :] = high
            z_l[at, :] = low
        return carry

    lax.fori_loop(0, 4, four_digits, 0)
    for half in range(2):
        at = slice(half * 256, (half + 1) * 256)
        image[:, at] = (
            dot(z_h[...], third_h[:, at])
            + dot(z_h[...], third_l[:, at])
            + dot(z_l[...], third_h[:, at])
        )
    for p2 in range(16):
        for group in range(4):
            out_ref[:, p2 * 512 + group * 128 : p2 * 512 + (group + 1) * 128] = jnp.concatenate(
                [
                    image[(group * 4 + k) * 16 : (group * 4 + k + 1) * 16, p2 * 32 : (p2 + 1) * 32]
                    for k in range(4)
                ],
                axis=1,
            )


def halo_kernel(image_ref, low_ref, high_ref, send_sem, recv_sem):
    flat = lax.axis_index("row") * NC + lax.axis_index("col")
    after, before = lax.rem(flat + 1, NR * NC), lax.rem(flat + NR * NC - 1, NR * NC)
    up = (after // NC, lax.rem(after, NC))
    down = (before // NC, lax.rem(before, NC))
    barrier = pltpu.get_barrier_semaphore()
    for peer in (up, down):
        pl.semaphore_signal(barrier, inc=1, device_id=peer, device_id_type=MESH)
    pl.semaphore_wait(barrier, 2)
    copies = [
        pltpu.make_async_remote_copy(
            image_ref, there, send_sem.at[i], recv_sem.at[i], device_id=peer, device_id_type=MESH
        )
        for i, (there, peer) in enumerate(((low_ref, up), (high_ref, down)))
    ]
    for copy in copies:
        copy.start()
    for copy in copies:
        copy.wait()


def smooth_kernel(edge_ref, taps_ref, own_ref, low_ref, high_ref, out_ref, across, band_h, band_l):
    mix = []
    for m in range(NSCALE):
        distance = lax.broadcasted_iota(jnp.int32, (16, 48), 1) - lax.broadcasted_iota(
            jnp.int32, (16, 48), 0
        )
        v = jnp.zeros((16, 48), F32)
        for t in range(KW):
            v = jnp.where(distance == t, taps_ref[m, t], v)
        mix.append(v)
    mix_h, mix_l = two_parts(jnp.concatenate(mix, axis=0))
    mix = jnp.concatenate([mix_h, mix_l, mix_h], axis=1)
    zero = jnp.zeros((NSCALE * 16, 128), F32)
    across[:, 0:128] = zero
    across[:, 128 + G : 256 + G] = zero

    no_low, no_high = edge_ref[0] == 0, edge_ref[0] == NR * NC - 1

    def cross(i, carry):
        here = pl.ds(pl.multiple_of(i * 512, 512), 512)
        below = jnp.where(no_low, 0.0, low_ref[:, here])
        above = jnp.where(no_high, 0.0, high_ref[:, here])
        high, low = two_parts(jnp.concatenate([below, own_ref[:, here], above], axis=0))
        across[:, pl.ds(pl.multiple_of(i * 512 + 128, 128), 512)] = dot(
            mix, jnp.concatenate([high, high, low], axis=0)
        )
        return carry

    lax.fori_loop(0, G // 512, cross, 0, unroll=2)
    band_h[...] = jnp.zeros_like(band_h)
    band_l[...] = jnp.zeros_like(band_l)
    difference = lax.broadcasted_iota(jnp.int32, (128, 128), 0) - lax.broadcasted_iota(
        jnp.int32, (128, 128), 1
    )
    for m in range(NSCALE):
        for k in range(3):
            distance = difference + (128 * k - 112)
            v = jnp.zeros((128, 128), F32)
            for t in range(KW):
                v = jnp.where(distance == t, taps_ref[m, t], v)
            high, low = two_parts(v)
            for o in range(2):
                at = slice((k + o) * 128, (k + o + 1) * 128)
                band_h[m, at, o * 128 : (o + 1) * 128] = high
                band_l[m, at, o * 128 : (o + 1) * 128] = low

    def along(i, carry):
        for m in range(NSCALE):
            window = jnp.concatenate(
                [
                    across[
                        m * 16 : (m + 1) * 16,
                        pl.ds(pl.multiple_of(i * 2048 + k * 256, 256), 512),
                    ]
                    for k in range(8)
                ],
                axis=0,
            )
            high, low = two_parts(window)
            done = dot(high, band_h[m]) + dot(low, band_h[m]) + dot(high, band_l[m])
            for k in range(8):
                out_ref[m, :, pl.ds(pl.multiple_of(i * 2048 + k * 256, 256), 256)] = done[
                    k * 16 : (k + 1) * 16
                ]
        return carry

    lax.fori_loop(0, G // 2048, along, 0)


def grid_subgrids(l0, group, vis, vis_pos, vis_w, grid_kernel, col):
    slot = 32 * (col % 4)
    pad = jnp.zeros((2, 128), F32)
    meta = lax.dynamic_update_slice(pad, jnp.stack([l0, group]).astype(F32), (0, slot))
    meta = jnp.concatenate([meta, jnp.zeros((6, 128), F32)], axis=0)
    return pl.pallas_call(
        gridding_kernel,
        out_shape=jax.ShapeDtypeStruct((NC * MSG, 128), F32),
        in_specs=[SM, VM, VM, VM, VM, VM],
        out_specs=VM,
        name="gridding",
    )(l0, vis, vis_pos, vis_w.reshape(1, -1), grid_kernel.T, meta)


def exchange_over_col(send):
    return pl.pallas_call(
        spread_kernel,
        out_shape=jax.ShapeDtypeStruct((NC, MSG, 128), F32),
        in_specs=[VM],
        out_specs=VM,
        scratch_shapes=[
            pltpu.SemaphoreType.DMA((NC,)),
            pltpu.SemaphoreType.DMA((NC,)),
            pltpu.SemaphoreType.DMA,
        ],
        compiler_params=pltpu.CompilerParams(collective_id=0, has_side_effects=True),
        name="spread",
    )(send)


def transform_rows(recv):
    tables = [jnp.asarray(t) for t in row_tables()]
    return pl.pallas_call(
        rows_kernel,
        out_shape=jax.ShapeDtypeStruct((NC * 128, 128), F32),
        in_specs=[VM] * 5,
        out_specs=VM,
        scratch_shapes=[
            pltpu.VMEM((2048, 256), BF),
            pltpu.VMEM((2048, 256), BF),
            pltpu.VMEM((1024, 256), BF),
            pltpu.VMEM((1024, 256), BF),
        ],
        name="rows",
    )(recv, *tables)


def exchange_all(send):
    return pl.pallas_call(
        turn_kernel,
        out_shape=jax.ShapeDtypeStruct((NC, NR, 4, 128), F32),
        in_specs=[VM],
        out_specs=VM,
        scratch_shapes=[
            pltpu.VMEM((NC, NR, 4, 128), F32),
            pltpu.SemaphoreType.DMA((NC,)),
            pltpu.SemaphoreType.DMA((NC,)),
            pltpu.SemaphoreType.DMA((NC, NR)),
            pltpu.SemaphoreType.DMA((NC, NR)),
            pltpu.SemaphoreType.DMA,
            pltpu.SemaphoreType.DMA((NC,)),
        ],
        compiler_params=pltpu.CompilerParams(collective_id=1, has_side_effects=True),
        name="turn",
    )(send.reshape(NC, NR, 4, 128))


def transform_columns(recv):
    tables = [jnp.asarray(t) for t in column_tables()]
    return pl.pallas_call(
        columns_kernel,
        out_shape=jax.ShapeDtypeStruct((16, G), F32),
        in_specs=[VM] * 8,
        out_specs=VM,
        scratch_shapes=[
            pltpu.VMEM((512, 512), BF),
            pltpu.VMEM((512, 512), BF),
            pltpu.VMEM((256, 1024), BF),
            pltpu.VMEM((256, 1024), BF),
            pltpu.VMEM((256, 512), F32),
        ],
        name="columns",
    )(recv.reshape(NC * NR * 4, 128), *tables)


def exchange_halo(image):
    side = jax.ShapeDtypeStruct((16, G), F32)
    return pl.pallas_call(
        halo_kernel,
        out_shape=(side, side),
        in_specs=[VM],
        out_specs=(VM, VM),
        scratch_shapes=[pltpu.SemaphoreType.DMA((2,)), pltpu.SemaphoreType.DMA((2,))],
        compiler_params=pltpu.CompilerParams(collective_id=2, has_side_effects=True),
        name="halo",
    )(image)


def smooth(image, low, high, scale_kernels):
    flat = lax.axis_index(("row", "col")).astype(jnp.int32)
    return pl.pallas_call(
        smooth_kernel,
        out_shape=jax.ShapeDtypeStruct((NSCALE, 16, G), F32),
        in_specs=[SM, SM, VM, VM, VM],
        out_specs=VM,
        scratch_shapes=[
            pltpu.VMEM((NSCALE * 16, G + 256), F32),
            pltpu.VMEM((NSCALE, 512, 256), BF),
            pltpu.VMEM((NSCALE, 512, 256), BF),
        ],
        name="smooth",
    )(flat.reshape(1), scale_kernels, image, low, high)


def per_device(
    vis, vis_pos, vis_w, subgrid_tile, subgrid_group, subgrid_col, grid_kernel, scale_kernels
):
    l0 = subgrid_tile[:, 0] * (G // NC) + subgrid_col
    send = grid_subgrids(
        l0, subgrid_group[:, 0], vis, vis_pos, vis_w, grid_kernel, lax.axis_index("col")
    )
    recv = exchange_over_col(send.reshape(NC, MSG, 128))
    turned = exchange_all(transform_rows(recv))
    image = transform_columns(turned)
    low, high = exchange_halo(image)
    return smooth(image, low, high, scale_kernels)


def solution(mesh):
    return jax.shard_map(
        per_device,
        mesh=mesh,
        in_specs=(
            P(None, ("row", "col")),
            P(None, ("row", "col")),
            P(("row", "col")),
            P(("row", "col"), None),
            P(("row", "col"), None),
            P(("row", "col")),
            P(),
            P(),
        ),
        out_specs=P(None, ("row", "col"), None),
        check_vma=False,
    )
```

```python
import functools
import math

import jax
import jax.numpy as jnp
import ml_dtypes
import numpy as np
from jax import lax
from jax.experimental import pallas as pl
from jax.experimental.pallas import tpu as pltpu
from jax.sharding import PartitionSpec as P

G = 8192
SUB = 32
SUP = 8
OVER = 8
VPS = 256
WSTEPS = 1024
KW = 33
NSCALE = 2
NR = 32
NC = 16
SD = 32
HALO = 16
HB = NR // 2
MSG = SD // 2 + 2

BF = jnp.bfloat16
F32 = jnp.float32
MESH = pl.DeviceIdType.MESH
NN = (((1,), (0,)), ((), ()))
NT = (((1,), (1,)), ((), ()))
VM = pl.BlockSpec(memory_space=pltpu.VMEM)
SM = pl.BlockSpec(memory_space=pltpu.SMEM)


def two_parts(x):
    high = x.astype(BF)
    return high, (x - high.astype(F32)).astype(BF)


def dot(a, b, dims=NN):
    return lax.dot_general(a, b, dims, preferred_element_type=F32)


def np_parts(x):
    x = np.asarray(x, np.float64)
    high = x.astype(np.float32).astype(ml_dtypes.bfloat16)
    low = (x - high.astype(np.float64)).astype(np.float32).astype(ml_dtypes.bfloat16)
    return high, low


def angle_tables(a, b, period):
    turn = 2.0 * math.pi * ((np.asarray(a, np.int64) * np.asarray(b, np.int64)) % period) / period
    return np.cos(turn), np.sin(turn)


def row_tables():
    q0 = np.arange(64)
    cos, sin = angle_tables(q0[:, None], q0[None, :], 64)
    first_h, first_l = np_parts(np.concatenate([cos, sin], 0))
    first = np.concatenate([first_h, first_l, first_h], 1)
    cos, sin = angle_tables(q0[:, None], np.arange(128)[None, :], G)
    twiddle = np.stack([cos, sin]).astype(np.float32)
    high = (4 * np.arange(NR)[None, :] + np.arange(4)[:, None]).reshape(-1)
    cos, sin = angle_tables(high[:, None], np.arange(128)[None, :], 128)
    second = np.concatenate(
        [np.concatenate([cos, -sin], 1), np.concatenate([sin, cos], 1)], 0
    )
    return (first, twiddle, *np_parts(second))


def column_tables():
    p0 = np.arange(NR)

    def first_matrix(bands):
        cos, sin = angle_tables(p0[:, None], bands[None, :], NR)
        full = np.concatenate([np.concatenate([cos, -sin], 1), np.concatenate([sin, cos], 1)], 0)
        high, low = np_parts(full)
        return np.concatenate([high, low, high], 1)

    band = np.arange(HB)
    first = np.stack([first_matrix(band), first_matrix(band[::-1]), first_matrix(band + 1)])
    i = np.arange(128) // 16
    cos, sin = angle_tables(p0[:, None], i[None, :], 256)
    turn_one = np.stack([cos, sin]).astype(np.float32)
    d = np.arange(8)
    cos, sin = angle_tables(d[:, None], d[None, :], 8)
    eye = np.eye(16)
    cos, sin = np.kron(cos, eye), np.kron(sin, eye)
    second = np.concatenate([np.concatenate([cos, -sin], 1), np.concatenate([sin, cos], 1)], 0)
    c, p0s = np.repeat(np.arange(NC), NR)[None, :], np.tile(p0, NC)[None, :]
    part = p0s + NR * d[:, None]
    turns = [angle_tables(part, 1, 512)]
    turns += [angle_tables(c, part + 256 * half, G) for half in range(2)]
    turn_two = np.concatenate([np.stack(t) for t in turns]).astype(np.float32)
    c = np.arange(NC)
    cos, sin = angle_tables(c[:, None], c[None, :], NC)
    eye = np.eye(NR)
    third = np.concatenate([np.kron(cos, eye), -np.kron(sin, eye)], 0) / G
    return (first, turn_one, *np_parts(second), turn_two, *np_parts(third))


ORDER_ONE = [(far, d) for d in (8, 7, 9, 6, 10, 5, 11, 4, 12, 3, 13, 2, 14, 1, 15) for far in (1, 0)]
ORDER_ONE = ORDER_ONE + [(1, 0)]
ORDER_TWO = (1, 15, 2, 14, 3, 13, 4, 12, 5, 11, 6, 10, 7, 9, 8)
SETS = 4
PER = NC // SETS
CHUNK = G // 4


def whole_kernel(names, *refs):
    r = dict(zip(names, refs))
    row, col = lax.axis_index("row"), lax.axis_index("col")
    half = row // HB
    barrier = pltpu.get_barrier_semaphore()
    flat = row * NC + col
    after, before = lax.rem(flat + 1, NR * NC), lax.rem(flat + NR * NC - 1, NR * NC)
    up = (after // NC, lax.rem(after, NC))
    down = (before // NC, lax.rem(before, NC))
    opposite = NR - 1 - row
    peers = [(row, lax.rem(col + d, NC)) for d in range(1, NC)]
    peers += [(opposite, lax.rem(col + d, NC)) for d in range(NC)]
    peers += [(lax.rem(row + e, NR), col) for e in range(1, NR)]
    peers += [up, down]
    for peer in peers:
        pl.semaphore_signal(barrier, inc=1, device_id=peer, device_id_type=MESH)
    tables = [
        pltpu.make_async_copy(r["hbm_" + n], r[n], r["table_sem"].at[i])
        for i, n in enumerate(TABLES)
    ]
    for table in tables:
        table.start()
    gridding(r, half)
    pl.semaphore_wait(barrier, len(peers))
    exchange_one(r, row, col, half, opposite)
    for table in tables:
        table.wait()
    rows(r, row, col)
    exchange_two(r, row, col)
    columns(r, row)
    smooth(r, flat, up, down)


def gridding(r, mirror):
    sign = 1 - 2 * mirror
    vis_ref, pos_ref, w_ref, rows_ref, out_ref = r["vis"], r["pos"], r["w"], r["rows"], r["send_one"]
    tap_axis = lax.broadcasted_iota(jnp.int32, (SUP, VPS), 0)
    columns = []
    for t in range(OVER):
        v = jnp.zeros((SUP, VPS), F32)
        for k in range(SUP):
            v = jnp.where(tap_axis == k, r["grid_taps"][t, k], v)
        columns.append(v)
    slot = lax.broadcasted_iota(jnp.int32, (SUB, VPS), 0)
    row_axis = jnp.where(
        mirror == 1, jnp.where((slot & 15) == 0, 16 - slot, 32 - slot), slot
    )
    col_axis = slot * sign
    shifted = jnp.where(lax.broadcasted_iota(jnp.int32, (NC, SUB), 0) == 0, mirror, 0)

    def weights(pos):
        step = jnp.broadcast_to(pos & (OVER - 1), (SUP, VPS))
        rows = columns[0]
        for t in range(1, OVER):
            rows = jnp.where(step == t, columns[t], rows)
        return rows

    def spread(rows, distance):
        out = jnp.zeros((SUB, VPS), F32)
        for t in range(SUP):
            out = jnp.where(distance == t, jnp.broadcast_to(rows[t : t + 1, :], (SUB, VPS)), out)
        return out

    def one(s):
        here = pl.ds(pl.multiple_of(s * VPS, VPS), VPS)
        pos_u, pos_v = pos_ref[0:1, here], pos_ref[1:2, here]
        angle = w_ref[0:1, here].astype(F32) * (2.0 * math.pi / WSTEPS)
        cosine, sine = jnp.cos(angle), jnp.sin(angle)
        real, imag = vis_ref[0:1, here], vis_ref[1:2, here]
        turned_real = real * cosine + imag * sine
        turned_imag = (imag * cosine - real * sine) * sign.astype(F32)
        along_u = spread(weights(pos_u), row_axis - lax.shift_right_logical(pos_u, 3))
        corner = r["col_s"][s] & (SUB - 1)
        corner = jnp.where(mirror == 1, 1 - corner, corner) & (SUB - 1)
        start = (31 * mirror - sign * corner) - lax.shift_right_logical(pos_v, 3)
        along_v = spread(weights(pos_v), (col_axis + start) & (SUB - 1))
        left_h, left_l = two_parts(
            jnp.concatenate([along_u * turned_real, along_u * turned_imag], axis=0)
        )
        right_h, right_l = two_parts(along_v)
        block = dot(left_h, right_h, NT) + dot(left_l, right_h, NT) + dot(left_h, right_l, NT)
        odd = ((shifted + r["group_s"][s]) & 1) == 1
        even_rows, odd_rows = [], []
        for ri in range(2):
            near, far = block[ri * 32 : ri * 32 + 16], block[ri * 32 + 16 : ri * 32 + 32]
            even_rows.append(jnp.where(odd, far, near))
            odd_rows.append(jnp.where(odd, near, far))
        return even_rows, odd_rows

    def pair(s, carry):
        here, there = one(s), one(s + SD // 2)
        for e in range(2):
            rows_ref[pl.ds(e * 256 + s, NC, stride=SD // 2), :] = jnp.concatenate(
                here[e] + there[e], axis=1
            )
        return carry

    lax.fori_loop(0, SD // 2, pair, 0)
    l0 = r["tile_v"][...] * (G // NC) + r["col_v"][...]
    l0 = jnp.where(mirror == 1, G - SUB + 1 - l0, l0).astype(F32)
    group = jnp.where(mirror == 1, 14 - r["group_v"][...], r["group_v"][...]).astype(F32)
    meta = jnp.concatenate(
        [jnp.concatenate([l0] * 4, axis=1), jnp.concatenate([group] * 4, axis=1)], axis=0
    )
    lane = lax.broadcasted_iota(jnp.int32, (2, 128), 1)
    mine = lax.shift_right_logical(lane, 5) == lax.rem(lax.axis_index("col"), 4)
    meta = jnp.where(mine, meta, 0.0)
    for k in range(2 * NC):
        out_ref[k, 0:16, :] = rows_ref[k * 16 : (k + 1) * 16, :]
        out_ref[k, 16:18, :] = meta


def exchange_one(r, row, col, half, opposite):
    send_ref, recv_ref = r["send_one"], r["recv_one"]

    def copy(far, d):
        to = lax.rem(col + d, NC)
        return pltpu.make_async_remote_copy(
            src_ref=send_ref.at[(1 - half if far else half) * NC + to],
            dst_ref=recv_ref.at[half * NC + col],
            send_sem=r["send_sem_one"].at[far, d],
            recv_sem=r["recv_sem_one"].at[far, d],
            device_id=(opposite if far else row, to),
            device_id_type=MESH,
        )

    for far, d in ORDER_ONE:
        copy(far, d).start()
    own = pltpu.make_async_copy(
        send_ref.at[half * NC + col], recv_ref.at[half * NC + col], r["own_sem"].at[0]
    )
    own.start()
    own.wait()
    for far, d in ORDER_ONE:
        copy(far, d).wait()


def rows(r, row, col):
    recv_ref, first_ref, turn_ref = r["recv_one"], r["first"], r["turn"]
    second_h, second_l, out_ref, extra_ref = r["second_h"], r["second_l"], r["send_two"], r["extra"]
    u_h, u_l, a_h, a_l = r["u_h"], r["u_l"], r["a_h"], r["a_l"]
    parity = row // HB
    shifted = jnp.where(col == 0, 1, 0)
    lane = lax.broadcasted_iota(jnp.int32, (SD, 128), 1)
    sub = lax.broadcasted_iota(jnp.int32, (SD, 128), 0)
    segment = lax.shift_right_logical(lane[0:16], 5)

    def unpack(z, carry):
        data = recv_ref[z, 0:16, :]
        corner = recv_ref[z, 16:17, :]
        mine = lane == sub + SD * (z & 3)
        l0 = jnp.sum(
            jnp.where(mine, jnp.broadcast_to(corner, (SD, 128)), 0.0), axis=1, keepdims=True
        )
        distance = lane - (l0.astype(jnp.int32) & 127)
        rolled = [data] + [pltpu.roll(data, SUB * k, 1) for k in range(1, 4)]
        wide = []
        for i in range(4):
            v = rolled[(0 - i) % 4]
            for p in range(1, 4):
                v = jnp.where(segment == p, rolled[(p - i) % 4], v)
            wide.append(v)
        real = jnp.concatenate([wide[0], wide[2]], axis=0)
        imag = jnp.concatenate([wide[1], wide[3]], axis=0)
        in_a = (distance >= 0) & (distance < SUB)
        in_b = distance < SUB - 128
        for ab, inside in enumerate((in_a, in_b)):
            high, low = two_parts(
                jnp.concatenate(
                    [jnp.where(inside, real, 0.0), jnp.where(inside, imag, 0.0)], axis=1
                )
            )
            at = pl.ds(pl.multiple_of(ab * 1024 + z * SD, SD), SD)
            u_h[at, :] = high
            u_l[at, :] = low
        return carry

    lax.fori_loop(0, 2 * NC, unpack, 0, unroll=2)

    index = []
    for group in range(8):
        corner = sum(recv_ref[group * 4 + i, 16:17, :] for i in range(4)).astype(jnp.int32)
        start = sum(recv_ref[group * 4 + i, 17:18, :] for i in range(4)).astype(jnp.int32)
        if group >= 4:
            start = start + shifted
        start = lax.shift_right_logical(start + ((start ^ parity) & 1), 1) * 64
        tile = lax.shift_right_logical(corner, 7)
        index.append((start + tile, start + ((tile + 1) & 63)))
    chunks = [
        jnp.concatenate([index[k][ab], index[k + 1][ab]], axis=1)
        for ab in range(2)
        for k in range(0, 8, 2)
    ]

    def placed(first, count):
        place = lax.broadcasted_iota(jnp.int32, (count, 256), 0) + first
        total = jnp.zeros((count, 256), F32)
        for k in range(8):
            pick = (place == chunks[k]).astype(F32).astype(BF)
            at = slice(k * 256, (k + 1) * 256)
            total = total + dot(pick, u_h[at, :]) + dot(pick, u_l[at, :])
        return total

    def inner(value):
        high, low = two_parts(value)
        both = dot(first_ref[...], jnp.concatenate([high, high, low], axis=0))
        real = both[:64, :128] - both[64:, 128:]
        imag = both[64:, :128] + both[:64, 128:]
        cos, sin = turn_ref[0], turn_ref[1]
        return two_parts(
            jnp.concatenate([real * cos - imag * sin, real * sin + imag * cos], axis=1)
        )

    def outer(high, low):
        return (
            dot(second_h[...], high, NT) + dot(second_l[...], high, NT) + dot(second_h[...], low, NT)
        )

    def four_rows(block, carry):
        total = placed(block * 256, 256)
        for k in range(4):
            high, low = inner(total[k * 64 : (k + 1) * 64])
            for cl in range(4):
                at = pl.ds(pl.multiple_of(cl * 128 + (block * 4 + k) * 16, 16), 16)
                a_h[at, :] = high[cl * 16 : (cl + 1) * 16]
                a_l[at, :] = low[cl * 16 : (cl + 1) * 16]
        return carry

    lax.fori_loop(0, 2, four_rows, 0)
    for pair in range(2):
        at = slice(pair * 256, (pair + 1) * 256)
        done = outer(a_h[at, :], a_l[at, :])
        for ri in range(2):
            for ch in range(4):
                for k in range(2):
                    for part in range(4):
                        r0 = ri * 128 + ch * 32 + part * 8
                        out_ref[
                            4 * ch + 2 * pair + k, pl.ds(part * 16 + ri, 8, stride=2), :
                        ] = done[r0 : r0 + 8, k * 128 : (k + 1) * 128]

    @pl.when(col == 0)
    def _():
        high, low = inner(placed(512, 64))
        done = outer(high, low)
        done = jnp.concatenate([done, jnp.zeros((256, 64), F32)], axis=1)
        where = lax.broadcasted_iota(jnp.int32, (8, 128), 1)
        where = lax.shift_right_logical(where, 4)
        for ch in range(4):
            for cl in range(4):
                v = jnp.zeros((8, 128), F32)
                for ri in range(2):
                    for part in range(4):
                        r0 = ri * 128 + ch * 32 + part * 8
                        to = part * 2 + ri
                        moved = pltpu.roll(done[r0 : r0 + 8], ((to - cl) * 16) % 128, 1)
                        v = jnp.where(where == to, moved, v)
                extra_ref[4 * ch + cl] = v

    @pl.when(col != 0)
    def _():
        extra_ref[...] = jnp.zeros_like(extra_ref)


def exchange_two(r, row, col):
    send_ref, mid_ref, out_ref = r["send_two"], r["mid"], r["recv_two"]
    extra_ref, relay_ref, all_ref = r["extra"], r["relay"], r["extras"]

    def first(d):
        to = lax.rem(col + d, NC)
        return pltpu.make_async_remote_copy(
            src_ref=send_ref.at[to],
            dst_ref=mid_ref.at[col],
            send_sem=r["send_a"].at[d],
            recv_sem=r["recv_a"].at[d],
            device_id=(row, to),
            device_id_type=MESH,
        )

    def extra(to):
        return pltpu.make_async_remote_copy(
            src_ref=extra_ref.at[to],
            dst_ref=relay_ref,
            send_sem=r["send_x"].at[to],
            recv_sem=r["recv_x"].at[0],
            device_id=(row, to),
            device_id_type=MESH,
        )

    def spread_extra(e):
        return pltpu.make_async_remote_copy(
            src_ref=relay_ref,
            dst_ref=all_ref.at[row],
            send_sem=r["send_y"].at[e],
            recv_sem=r["recv_y"].at[e],
            device_id=(lax.rem(row + e, NR), col),
            device_id_type=MESH,
        )

    def second(g, e):
        to = lax.rem(row + e, NR)
        return pltpu.make_async_remote_copy(
            src_ref=mid_ref.at[pl.ds(g * PER, PER), pl.ds(2 * to, 2)],
            dst_ref=out_ref.at[pl.ds(g * PER, PER), pl.ds(2 * row, 2)],
            send_sem=r["send_b"].at[g, e],
            recv_sem=r["recv_b"].at[g, e],
            device_id=(to, col),
            device_id_type=MESH,
        )

    def keep(g):
        return pltpu.make_async_copy(
            mid_ref.at[pl.ds(g * PER, PER), pl.ds(2 * row, 2)],
            out_ref.at[pl.ds(g * PER, PER), pl.ds(2 * row, 2)],
            r["own_b"].at[g],
        )

    for d in ORDER_TWO[:4]:
        first(d).start()

    @pl.when(col == 0)
    def _():
        for d in range(1, NC):
            extra(d).start()

    for d in ORDER_TWO[4:]:
        first(d).start()
    own = pltpu.make_async_copy(send_ref.at[col], mid_ref.at[col], r["recv_a"].at[0])
    own.start()

    @pl.when(col == 0)
    def _():
        mine = pltpu.make_async_copy(extra_ref.at[0], relay_ref, r["recv_x"].at[1])
        mine.start()
        mine.wait()

    @pl.when(col != 0)
    def _():
        extra(0).wait_recv()

    mine = pltpu.make_async_copy(relay_ref, all_ref.at[row], r["send_y"].at[0])
    mine.start()
    mine.wait()
    sets = [lax.rem(col // PER + k, SETS) for k in (0, 1, 3, 2)]
    for i, g in enumerate(sets):
        for k in range(PER):
            first(lax.rem(col - (g * PER + k) + NC, NC)).wait_recv()
        keep(g).start()

        def go(e, carry, g=g):
            second(g, e).start()
            return carry

        lax.fori_loop(1, NR, go, 0)
        if i == 1:

            def go_extra(e, carry):
                spread_extra(e).start()
                return carry

            lax.fori_loop(1, NR, go_extra, 0)
    for d in ORDER_TWO:
        first(d).wait_send()

    @pl.when(col == 0)
    def _():
        for d in range(1, NC):
            extra(d).wait_send()

    def end_extra(e, carry):
        spread_extra(e).wait()
        return carry

    lax.fori_loop(1, NR, end_extra, 0)
    for g in sets:
        keep(g).wait()

        def end(e, carry, g=g):
            second(g, e).wait()
            return carry

        lax.fori_loop(1, NR, end, 0)


def columns(r, row):
    in_ref, extra_ref, first_ref, turn_one = r["recv_two"], r["extras"], r["col_first"], r["turn_one"]
    second_h, second_l, turn_two = r["mix_h"], r["mix_l"], r["turn_two"]
    y_h, y_l, middle, z_h, z_l = r["y_h"], r["y_l"], r["middle"], r["z_h"], r["z_l"]
    lane = lax.broadcasted_iota(jnp.int32, (HB, 128), 1)
    held = extra_ref[0:HB, lax.rem(row, 8), :]
    mine = held
    for k in range(1, 4):
        mine = jnp.where(row // 8 == k, pltpu.roll(held, 128 - 32 * k, 1), mine)
    real = jnp.where(lane < 16, mine, 0.0)
    imag = jnp.where(lane < 16, pltpu.roll(mine, 112, 1), 0.0)
    high, low = two_parts(jnp.concatenate([real, imag], axis=0))
    added = dot(first_ref[2], jnp.concatenate([high, high, low], axis=0))
    added = jnp.concatenate([added, jnp.zeros_like(added)], axis=1)

    def two(pair, carry):
        for e in range(2):

            def piece(ri, pair=pair, e=e):
                return jnp.concatenate(
                    [
                        in_ref[pair * 2 + k, pl.ds(e * 32 + ri, HB, stride=2), :]
                        for k in range(2)
                    ],
                    axis=1,
                )

            high, low = two_parts(jnp.concatenate([piece(0), piece(1)], axis=0))
            done = dot(first_ref[e], jnp.concatenate([high, high, low], axis=0))
            if e == 0:
                done = done + jnp.where(pair == 0, added, 0.0)
            cos, sin = turn_one[0], turn_one[1]
            for k in range(2):
                real = done[:NR, k * 128 : (k + 1) * 128]
                imag = done[NR:, k * 128 : (k + 1) * 128]
                high, low = two_parts(
                    jnp.concatenate([real * cos - imag * sin, real * sin + imag * cos], axis=1)
                )
                at = pl.ds(pl.multiple_of(e * 512 + (pair * 2 + k) * NR, NR), NR)
                y_h[at, :] = high
                y_l[at, :] = low
        return carry

    lax.fori_loop(0, NC // 2, two, 0)

    def digits(n, carry):
        at = pl.ds(pl.multiple_of(n * 256, 256), 256)
        middle[:, at] = (
            dot(second_h[...], y_h[at, :], NT)
            + dot(second_l[...], y_h[at, :], NT)
            + dot(second_h[...], y_l[at, :], NT)
        )
        return carry

    lax.fori_loop(0, 4, digits, 0)

    def butterfly(p1, carry):
        at = pl.ds(pl.multiple_of(p1 * 16, 16), 16)
        below = pl.ds(pl.multiple_of(128 + p1 * 16, 16), 16)

        def factor(k):
            return turn_two[k, pl.ds(p1, 1), :]

        real, imag = middle[at, 0:512], middle[below, 0:512]
        other_real, other_imag = middle[at, 512:1024], middle[below, 512:1024]
        cos, sin = factor(0), factor(1)
        other_real, other_imag = (
            other_real * cos - other_imag * sin,
            other_real * sin + other_imag * cos,
        )
        for half in range(2):
            if half == 0:
                one, two_ = real + other_real, imag + other_imag
            else:
                one, two_ = real - other_real, imag - other_imag
            cos, sin = factor(2 + 2 * half), factor(3 + 2 * half)
            high, low = two_parts(
                jnp.concatenate([one * cos - two_ * sin, one * sin + two_ * cos], axis=1)
            )
            to = pl.ds(pl.multiple_of(half * 128 + p1 * 16, 16), 16)
            z_h[to, :] = high
            z_l[to, :] = low
        return carry

    lax.fori_loop(0, 8, butterfly, 0)


def smooth(r, flat, up, down):
    image, third_h, third_l, z_h, z_l = r["image"], r["third_h"], r["third_l"], r["z_h"], r["z_l"]
    own_ref, low_ref, high_ref, taps_ref = r["own"], r["low"], r["high"], r["taps"]
    across, band_h, band_l, result = r["across"], r["band_h"], r["band_l"], r["result"]

    def sides(chunk):
        at = pl.ds(chunk * CHUNK, CHUNK)
        return [
            pltpu.make_async_remote_copy(
                own_ref.at[:, at],
                there.at[:, at],
                r["send_h"].at[i, chunk],
                r["recv_h"].at[i, chunk],
                device_id=peer,
                device_id_type=MESH,
            )
            for i, (there, peer) in enumerate(((low_ref, up), (high_ref, down)))
        ]

    for half in range(2):
        at = slice(half * 256, (half + 1) * 256)
        image[:, at] = (
            dot(z_h[...], third_h[:, at])
            + dot(z_h[...], third_l[:, at])
            + dot(z_l[...], third_h[:, at])
        )
        for p2 in range(half * 8, half * 8 + 8):
            for group in range(4):
                own_ref[:, p2 * 512 + group * 128 : p2 * 512 + (group + 1) * 128] = (
                    jnp.concatenate(
                        [
                            image[
                                (group * 4 + k) * 16 : (group * 4 + k + 1) * 16,
                                p2 * 32 : (p2 + 1) * 32,
                            ]
                            for k in range(4)
                        ],
                        axis=1,
                    )
                )
            if p2 % 4 == 3:
                for copy in sides(p2 // 4):
                    copy.start()

    mix = []
    for m in range(NSCALE):
        distance = lax.broadcasted_iota(jnp.int32, (16, 48), 1) - lax.broadcasted_iota(
            jnp.int32, (16, 48), 0
        )
        v = jnp.zeros((16, 48), F32)
        for t in range(KW):
            v = jnp.where(distance == t, taps_ref[m, t], v)
        mix.append(v)
    mix_h, mix_l = two_parts(jnp.concatenate(mix, axis=0))
    mix = jnp.concatenate([mix_h, mix_l, mix_h], axis=1)
    zero = jnp.zeros((NSCALE * 16, 128), F32)
    across[:, 0:128] = zero
    across[:, 128 + G : 256 + G] = zero
    band_h[...] = jnp.zeros_like(band_h)
    band_l[...] = jnp.zeros_like(band_l)
    difference = lax.broadcasted_iota(jnp.int32, (128, 128), 0) - lax.broadcasted_iota(
        jnp.int32, (128, 128), 1
    )
    for m in range(NSCALE):
        for k in range(3):
            distance = difference + (128 * k - 112)
            v = jnp.zeros((128, 128), F32)
            for t in range(KW):
                v = jnp.where(distance == t, taps_ref[m, t], v)
            high, low = two_parts(v)
            for o in range(2):
                at = slice((k + o) * 128, (k + o + 1) * 128)
                band_h[m, at, o * 128 : (o + 1) * 128] = high
                band_l[m, at, o * 128 : (o + 1) * 128] = low

    no_low, no_high = flat == 0, flat == NR * NC - 1

    def cross(i):
        here = slice(i * 512, (i + 1) * 512)
        below = jnp.where(no_low, 0.0, low_ref[:, here])
        above = jnp.where(no_high, 0.0, high_ref[:, here])
        high, low = two_parts(jnp.concatenate([below, own_ref[:, here], above], axis=0))
        across[:, i * 512 + 128 : i * 512 + 640] = dot(
            mix, jnp.concatenate([high, high, low], axis=0)
        )

    def leave(i):
        at = pl.ds(i * CHUNK, CHUNK)
        return pltpu.make_async_copy(
            result.at[:, :, at], r["out"].at[:, :, at], r["out_sem"].at[i]
        )

    def along(i):
        for m in range(NSCALE):
            window = jnp.concatenate(
                [
                    across[m * 16 : (m + 1) * 16, i * CHUNK + k * 256 : i * CHUNK + k * 256 + 512]
                    for k in range(8)
                ],
                axis=0,
            )
            high, low = two_parts(window)
            done = dot(high, band_h[m]) + dot(low, band_h[m]) + dot(high, band_l[m])
            for k in range(8):
                result[m, :, i * CHUNK + k * 256 : i * CHUNK + (k + 1) * 256] = done[
                    k * 16 : (k + 1) * 16
                ]
        leave(i).start()

    for chunk in range(4):
        for copy in sides(chunk):
            copy.wait_recv()
        for i in range(4):
            cross(chunk * 4 + i)
        if chunk:
            along(chunk - 1)
    along(3)
    for chunk in range(4):
        for copy in sides(chunk):
            copy.wait_send()
        leave(chunk).wait()


TABLES = [
    "first", "turn", "second_h", "second_l", "col_first", "turn_one", "mix_h", "mix_l",
    "turn_two", "third_h", "third_l",
]


def per_device(
    vis, vis_pos, vis_w, subgrid_tile, subgrid_group, subgrid_col, grid_kernel, scale_kernels
):
    tile, group = subgrid_tile[:, 0], subgrid_group[:, 0]
    tables = list(row_tables()) + list(column_tables())
    inputs = {
        "group_s": (SM, group),
        "col_s": (SM, subgrid_col),
        "grid_taps": (SM, grid_kernel),
        "taps": (SM, scale_kernels),
        "vis": (VM, vis),
        "pos": (VM, vis_pos),
        "w": (VM, vis_w.reshape(1, -1)),
        "tile_v": (VM, tile.reshape(1, -1)),
        "group_v": (VM, group.reshape(1, -1)),
        "col_v": (VM, subgrid_col.reshape(1, -1)),
    }
    for name, table in zip(TABLES, tables):
        inputs["hbm_" + name] = (pl.BlockSpec(memory_space=pl.ANY), jnp.asarray(table))
    dma = pltpu.SemaphoreType.DMA
    scratch = {name: pltpu.VMEM(t.shape, t.dtype) for name, t in zip(TABLES, tables)}
    scratch |= {
        "table_sem": dma((len(TABLES),)),
        "rows": pltpu.VMEM((512, 128), F32),
        "send_one": pltpu.VMEM((2 * NC, MSG, 128), F32),
        "recv_one": pltpu.VMEM((2 * NC, MSG, 128), F32),
        "send_sem_one": dma((2, NC)),
        "recv_sem_one": dma((2, NC)),
        "own_sem": dma((1,)),
        "u_h": pltpu.VMEM((2048, 256), BF),
        "u_l": pltpu.VMEM((2048, 256), BF),
        "a_h": pltpu.VMEM((512, 256), BF),
        "a_l": pltpu.VMEM((512, 256), BF),
        "send_two": pltpu.VMEM((NC, 2 * NR, 128), F32),
        "extra": pltpu.VMEM((NC, 8, 128), F32),
        "mid": pltpu.VMEM((NC, 2 * NR, 128), F32),
        "relay": pltpu.VMEM((8, 128), F32),
        "recv_two": pltpu.VMEM((NC, 2 * NR, 128), F32),
        "extras": pltpu.VMEM((NR, 8, 128), F32),
        "send_a": dma((NC,)),
        "recv_a": dma((NC,)),
        "send_x": dma((NC,)),
        "recv_x": dma((2,)),
        "send_y": dma((NR,)),
        "recv_y": dma((NR,)),
        "send_b": dma((SETS, NR)),
        "recv_b": dma((SETS, NR)),
        "own_b": dma((SETS,)),
        "y_h": pltpu.VMEM((1024, 256), BF),
        "y_l": pltpu.VMEM((1024, 256), BF),
        "middle": pltpu.VMEM((256, 1024), F32),
        "z_h": pltpu.VMEM((256, 1024), BF),
        "z_l": pltpu.VMEM((256, 1024), BF),
        "image": pltpu.VMEM((256, 512), F32),
        "own": pltpu.VMEM((16, G), F32),
        "low": pltpu.VMEM((16, G), F32),
        "high": pltpu.VMEM((16, G), F32),
        "send_h": dma((2, 4)),
        "recv_h": dma((2, 4)),
        "across": pltpu.VMEM((NSCALE * 16, G + 256), F32),
        "band_h": pltpu.VMEM((NSCALE, 512, 256), BF),
        "band_l": pltpu.VMEM((NSCALE, 512, 256), BF),
        "result": pltpu.VMEM((NSCALE, 16, G), F32),
        "out_sem": dma((4,)),
    }
    names = list(inputs) + ["out"] + list(scratch)
    return pl.pallas_call(
        functools.partial(whole_kernel, names),
        out_shape=jax.ShapeDtypeStruct((NSCALE, 16, G), F32),
        in_specs=[spec for spec, _ in inputs.values()],
        out_specs=pl.BlockSpec(memory_space=pl.ANY),
        scratch_shapes=list(scratch.values()),
        compiler_params=pltpu.CompilerParams(collective_id=0, has_side_effects=True),
        name="whole",
    )(*[value for _, value in inputs.values()])


def solution(mesh):
    return jax.shard_map(
        per_device,
        mesh=mesh,
        in_specs=(
            P(None, ("row", "col")),
            P(None, ("row", "col")),
            P(("row", "col")),
            P(("row", "col"), None),
            P(("row", "col"), None),
            P(("row", "col")),
            P(),
            P(),
        ),
        out_specs=P(None, ("row", "col"), None),
        check_vma=False,
    )
```

```python
import functools
import math
import types

import jax
import jax.numpy as jnp
import ml_dtypes
import numpy as np
from jax import lax
from jax.experimental import pallas as pl
from jax.experimental.pallas import tpu as pltpu
from jax.sharding import PartitionSpec as P

G = 8192
SUB = 32
SUP = 8
OVER = 8
VPS = 256
WSTEPS = 1024
KW = 33
NSCALE = 2
NR = 32
NC = 16
SD = 32
HALO = 16
HB = NR // 2
MSG = SD // 2 + 2

BF = jnp.bfloat16
F32 = jnp.float32
MESH = pl.DeviceIdType.MESH
NN = (((1,), (0,)), ((), ()))
NT = (((1,), (1,)), ((), ()))
VM = pl.BlockSpec(memory_space=pltpu.VMEM)
SM = pl.BlockSpec(memory_space=pltpu.SMEM)
ANY = pl.BlockSpec(memory_space=pl.ANY)


def two_parts(x):
    high = x.astype(BF)
    return high, (x - high.astype(F32)).astype(BF)


def dot(a, b, dims=NN):
    return lax.dot_general(a, b, dims, preferred_element_type=F32)


def np_parts(x):
    x = np.asarray(x, np.float64)
    high = x.astype(np.float32).astype(ml_dtypes.bfloat16)
    low = (x - high.astype(np.float64)).astype(np.float32).astype(ml_dtypes.bfloat16)
    return high, low


def angle_tables(a, b, period):
    turn = 2.0 * math.pi * ((np.asarray(a, np.int64) * np.asarray(b, np.int64)) % period) / period
    return np.cos(turn), np.sin(turn)


def row_tables():
    q0 = np.arange(64)
    cos, sin = angle_tables(q0[:, None], q0[None, :], 64)
    first_h, first_l = np_parts(np.concatenate([cos, sin], 0))
    first = np.concatenate([first_h, first_l, first_h], 1)
    cos, sin = angle_tables(q0[:, None], np.arange(128)[None, :], G)
    twiddle = np.stack([cos, sin]).astype(np.float32)
    high = (4 * np.arange(NR)[None, :] + np.arange(4)[:, None]).reshape(-1)
    cos, sin = angle_tables(high[:, None], np.arange(128)[None, :], 128)
    second = np.concatenate(
        [np.concatenate([cos, -sin], 1), np.concatenate([sin, cos], 1)], 0
    )
    return (first, twiddle, *np_parts(second))


def column_tables():
    p0 = np.arange(NR)

    def first_matrix(bands):
        cos, sin = angle_tables(p0[:, None], bands[None, :], NR)
        full = np.concatenate([np.concatenate([cos, -sin], 1), np.concatenate([sin, cos], 1)], 0)
        high, low = np_parts(full)
        return np.concatenate([high, low, high], 1)

    band = np.arange(HB)
    first = np.stack([first_matrix(band), first_matrix(band[::-1]), first_matrix(band + 1)])
    i = np.arange(128) // 16
    cos, sin = angle_tables(p0[:, None], i[None, :], 256)
    turn_one = np.stack([cos, sin]).astype(np.float32)
    d = np.arange(8)
    cos, sin = angle_tables(d[:, None], d[None, :], 8)
    eye = np.eye(16)
    cos, sin = np.kron(cos, eye), np.kron(sin, eye)
    second = np.concatenate([np.concatenate([cos, -sin], 1), np.concatenate([sin, cos], 1)], 0)
    c, p0s = np.repeat(np.arange(NC), NR)[None, :], np.tile(p0, NC)[None, :]
    part = p0s + NR * d[:, None]
    turns = [angle_tables(part, 1, 512)]
    turns += [angle_tables(c, part + 256 * half, G) for half in range(2)]
    turn_two = np.concatenate([np.stack(t) for t in turns]).astype(np.float32)
    c = np.arange(NC)
    cos, sin = angle_tables(c[:, None], c[None, :], NC)
    eye = np.eye(NR)
    third = np.concatenate([np.kron(cos, eye), -np.kron(sin, eye)], 0) / G
    return (first, turn_one, *np_parts(second), turn_two, *np_parts(third))


ORDER_ONE = [(far, d) for d in (8, 7, 9, 6, 10, 5, 11, 4, 12, 3, 13, 2, 14, 1, 15) for far in (1, 0)]
ORDER_ONE = ORDER_ONE + [(1, 0)]
ORDER_TWO = (1, 15, 2, 14, 3, 13, 4, 12, 5, 11, 6, 10, 7, 9, 8)
SETS = 4
PER = NC // SETS
CHUNK = G // 4


def landed(ref, other, sem):
    pltpu.make_async_copy(other, ref, sem).wait()


def whole_kernel(names, *refs):
    r = types.SimpleNamespace(**dict(zip(names, refs)))
    row, col = lax.axis_index("row"), lax.axis_index("col")
    half = row // HB
    barrier = pltpu.get_barrier_semaphore()
    flat = row * NC + col
    after, before = lax.rem(flat + 1, NR * NC), lax.rem(flat + NR * NC - 1, NR * NC)
    up = (after // NC, lax.rem(after, NC))
    down = (before // NC, lax.rem(before, NC))
    opposite = NR - 1 - row
    peers = [(row, lax.rem(col + d, NC)) for d in range(1, NC)]
    peers += [(opposite, lax.rem(col + d, NC)) for d in range(NC)]
    peers += [(lax.rem(row + e, NR), col) for e in range(1, NR)]
    peers += [up, down]
    given = [
        pltpu.make_async_copy(getattr(r, PRE + n), getattr(r, n), r.given_sem.at[i])
        for i, n in enumerate(GIVEN)
    ]
    for copy in given:
        copy.start()
    for peer in peers:
        pl.semaphore_signal(barrier, inc=1, device_id=peer, device_id_type=MESH)
    tables = [
        pltpu.make_async_copy(getattr(r, PRE + n), getattr(r, n), r.table_sem.at[i])
        for i, n in enumerate(TABLES)
    ]
    for table in tables:
        table.start()
    for copy in given:
        copy.wait()
    gridding(r, half)
    pl.semaphore_wait(barrier, len(peers))
    exchange_one(r, row, col, half, opposite)
    for table in tables:
        table.wait()
    past_end = rows(r, row, col)
    arrived = exchange_two(r, row, col, past_end)
    columns(r, row, arrived)
    smooth(r, flat, up, down)
    finish(r, col)


def gridding(r, mirror):
    sign = 1 - 2 * mirror
    vis_ref, pos_ref, w_ref, rows_ref, out_ref = r.vis, r.pos, r.w, r.rows, r.send_one
    tap_axis = lax.broadcasted_iota(jnp.int32, (SUP, VPS), 0)
    columns = []
    for t in range(OVER):
        v = jnp.zeros((SUP, VPS), F32)
        for k in range(SUP):
            v = jnp.where(tap_axis == k, r.grid_taps[t, k], v)
        columns.append(v)
    slot = lax.broadcasted_iota(jnp.int32, (SUB, VPS), 0)
    row_axis = jnp.where(
        mirror == 1, jnp.where((slot & 15) == 0, 16 - slot, 32 - slot), slot
    )
    col_axis = slot * sign
    shifted = jnp.where(lax.broadcasted_iota(jnp.int32, (NC, SUB), 0) == 0, mirror, 0)

    def weights(pos):
        step = jnp.broadcast_to(pos & (OVER - 1), (SUP, VPS))
        rows = columns[0]
        for t in range(1, OVER):
            rows = jnp.where(step == t, columns[t], rows)
        return rows

    def spread(rows, distance):
        out = jnp.zeros((SUB, VPS), F32)
        for t in range(SUP):
            out = jnp.where(distance == t, jnp.broadcast_to(rows[t : t + 1, :], (SUB, VPS)), out)
        return out

    def one(s):
        here = pl.ds(pl.multiple_of(s * VPS, VPS), VPS)
        pos_u, pos_v = pos_ref[0:1, here], pos_ref[1:2, here]
        angle = w_ref[0:1, here].astype(F32) * (2.0 * math.pi / WSTEPS)
        cosine, sine = jnp.cos(angle), jnp.sin(angle)
        real, imag = vis_ref[0:1, here], vis_ref[1:2, here]
        turned_real = real * cosine + imag * sine
        turned_imag = (imag * cosine - real * sine) * sign.astype(F32)
        along_u = spread(weights(pos_u), row_axis - lax.shift_right_logical(pos_u, 3))
        corner = r.col_s[s] & (SUB - 1)
        corner = jnp.where(mirror == 1, 1 - corner, corner) & (SUB - 1)
        start = (31 * mirror - sign * corner) - lax.shift_right_logical(pos_v, 3)
        along_v = spread(weights(pos_v), (col_axis + start) & (SUB - 1))
        left_h, left_l = two_parts(
            jnp.concatenate([along_u * turned_real, along_u * turned_imag], axis=0)
        )
        right_h, right_l = two_parts(along_v)
        block = dot(left_h, right_h, NT) + dot(left_l, right_h, NT) + dot(left_h, right_l, NT)
        odd = ((shifted + r.group_s[s]) & 1) == 1
        even_rows, odd_rows = [], []
        for ri in range(2):
            near, far = block[ri * 32 : ri * 32 + 16], block[ri * 32 + 16 : ri * 32 + 32]
            even_rows.append(jnp.where(odd, far, near))
            odd_rows.append(jnp.where(odd, near, far))
        return even_rows, odd_rows

    def pair(s, carry):
        here, there = one(s), one(s + SD // 2)
        for e in range(2):
            rows_ref[pl.ds(e * 256 + s, NC, stride=SD // 2), :] = jnp.concatenate(
                here[e] + there[e], axis=1
            )
        return carry

    lax.fori_loop(0, SD // 2, pair, 0)
    l0 = r.tile_v[...] * (G // NC) + r.col_v[...]
    l0 = jnp.where(mirror == 1, G - SUB + 1 - l0, l0).astype(F32)
    group = jnp.where(mirror == 1, 14 - r.group_v[...], r.group_v[...]).astype(F32)
    meta = jnp.concatenate(
        [jnp.concatenate([l0] * 4, axis=1), jnp.concatenate([group] * 4, axis=1)], axis=0
    )
    lane = lax.broadcasted_iota(jnp.int32, (2, 128), 1)
    mine = lax.shift_right_logical(lane, 5) == lax.rem(lax.axis_index("col"), 4)
    meta = jnp.where(mine, meta, 0.0)
    for k in range(2 * NC):
        out_ref[k, 0:16, :] = rows_ref[k * 16 : (k + 1) * 16, :]
        out_ref[k, 16:18, :] = meta


def unpack(r, z):
    recv_ref, u_h, u_l = r.recv_one, r.u_h, r.u_l
    lane = lax.broadcasted_iota(jnp.int32, (SD, 128), 1)
    sub = lax.broadcasted_iota(jnp.int32, (SD, 128), 0)
    segment = lax.shift_right_logical(lane[0:16], 5)
    data = recv_ref[z, 0:16, :]
    corner = recv_ref[z, 16:17, :]
    mine = lane == sub + SD * (z & 3)
    l0 = jnp.sum(
        jnp.where(mine, jnp.broadcast_to(corner, (SD, 128)), 0.0), axis=1, keepdims=True
    )
    distance = lane - (l0.astype(jnp.int32) & 127)
    rolled = [data] + [pltpu.roll(data, SUB * k, 1) for k in range(1, 4)]
    wide = []
    for i in range(4):
        v = rolled[(0 - i) % 4]
        for p in range(1, 4):
            v = jnp.where(segment == p, rolled[(p - i) % 4], v)
        wide.append(v)
    real = jnp.concatenate([wide[0], wide[2]], axis=0)
    imag = jnp.concatenate([wide[1], wide[3]], axis=0)
    in_a = (distance >= 0) & (distance < SUB)
    in_b = distance < SUB - 128
    for ab, inside in enumerate((in_a, in_b)):
        high, low = two_parts(
            jnp.concatenate(
                [jnp.where(inside, real, 0.0), jnp.where(inside, imag, 0.0)], axis=1
            )
        )
        at = pl.ds(pl.multiple_of(ab * 1024 + z * SD, SD), SD)
        u_h[at, :] = high
        u_l[at, :] = low


def exchange_one(r, row, col, half, opposite):
    send_ref, recv_ref = r.send_one, r.recv_one

    def copy(far, d):
        to = lax.rem(col + d, NC)
        there = half + far * (1 - 2 * half)
        return pltpu.make_async_remote_copy(
            src_ref=send_ref.at[there * NC + to],
            dst_ref=recv_ref.at[half * NC + col],
            send_sem=r.send_sem_one.at[0],
            recv_sem=r.recv_sem_one.at[far, d],
            device_id=(row + far * (opposite - row), to),
            device_id_type=MESH,
        )

    for far, d in ORDER_ONE:
        copy(far, d).start()
    own = pltpu.make_async_copy(
        send_ref.at[half * NC + col], recv_ref.at[half * NC + col], r.own_sem.at[0]
    )
    own.start()
    own.wait()
    unpack(r, half * NC + col)

    def arrive(i, carry):
        step = i // 2
        far = 1 - lax.rem(i, 2)
        d = 8 + ((step + 1) // 2) * (1 - 2 * lax.rem(step, 2))
        copy(far, d).wait_recv()
        there = half + far * (1 - 2 * half)
        unpack(r, there * NC + lax.rem(col + NC - d, NC))
        return carry

    lax.fori_loop(0, 2 * NC - 1, arrive, 0)


def rows(r, row, col):
    recv_ref, first_ref, turn_ref = r.recv_one, r.first, r.turn
    second_h, second_l, out_ref, extra_ref = r.second_h, r.second_l, r.send_two, r.extra
    u_h, u_l, a_h, a_l = r.u_h, r.u_l, r.a_h, r.a_l
    parity = row // HB
    shifted = jnp.where(col == 0, 1, 0)
    index = []
    for group in range(8):
        corner = sum(recv_ref[group * 4 + i, 16:17, :] for i in range(4)).astype(jnp.int32)
        start = sum(recv_ref[group * 4 + i, 17:18, :] for i in range(4)).astype(jnp.int32)
        if group >= 4:
            start = start + shifted
        start = lax.shift_right_logical(start + ((start ^ parity) & 1), 1) * 64
        tile = lax.shift_right_logical(corner, 7)
        index.append((start + tile, start + ((tile + 1) & 63)))
    chunks = [
        jnp.concatenate([index[k][ab], index[k + 1][ab]], axis=1)
        for ab in range(2)
        for k in range(0, 8, 2)
    ]

    def placed(first, count):
        place = lax.broadcasted_iota(jnp.int32, (count, 256), 0) + first
        total = jnp.zeros((count, 256), F32)
        for k in range(8):
            pick = (place == chunks[k]).astype(F32).astype(BF)
            at = slice(k * 256, (k + 1) * 256)
            total = total + dot(pick, u_h[at, :]) + dot(pick, u_l[at, :])
        return total

    def inner(value):
        high, low = two_parts(value)
        both = dot(first_ref[...], jnp.concatenate([high, high, low], axis=0))
        real = both[:64, :128] - both[64:, 128:]
        imag = both[64:, :128] + both[:64, 128:]
        cos, sin = turn_ref[0], turn_ref[1]
        return two_parts(
            jnp.concatenate([real * cos - imag * sin, real * sin + imag * cos], axis=1)
        )

    def outer(high, low):
        return (
            dot(second_h[...], high, NT) + dot(second_l[...], high, NT) + dot(second_h[...], low, NT)
        )

    def four_rows(block, carry):
        total = placed(block * 256, 256)
        for k in range(4):
            high, low = inner(total[k * 64 : (k + 1) * 64])
            for cl in range(4):
                at = pl.ds(pl.multiple_of(cl * 128 + (block * 4 + k) * 16, 16), 16)
                a_h[at, :] = high[cl * 16 : (cl + 1) * 16]
                a_l[at, :] = low[cl * 16 : (cl + 1) * 16]
        return carry

    lax.fori_loop(0, 2, four_rows, 0)
    for pair in range(2):
        at = slice(pair * 256, (pair + 1) * 256)
        done = outer(a_h[at, :], a_l[at, :])
        for ri in range(2):
            for ch in range(4):
                for k in range(2):
                    for part in range(4):
                        r0 = ri * 128 + ch * 32 + part * 8
                        out_ref[
                            4 * ch + 2 * pair + k, pl.ds(part * 16 + ri, 8, stride=2), :
                        ] = done[r0 : r0 + 8, k * 128 : (k + 1) * 128]

    def past_end():
        high, low = inner(placed(512, 64))
        done = outer(high, low)
        done = jnp.concatenate([done, jnp.zeros((256, 64), F32)], axis=1)
        where = lax.broadcasted_iota(jnp.int32, (8, 128), 1)
        where = lax.shift_right_logical(where, 4)
        for ch in range(4):
            for cl in range(4):
                v = jnp.zeros((8, 128), F32)
                for ri in range(2):
                    for part in range(4):
                        r0 = ri * 128 + ch * 32 + part * 8
                        to = part * 2 + ri
                        moved = pltpu.roll(done[r0 : r0 + 8], ((to - cl) * 16) % 128, 1)
                        v = jnp.where(where == to, moved, v)
                extra_ref[4 * ch + cl] = v

    return past_end


def exchange_two(r, row, col, past_end):
    send_ref, mid_ref, out_ref = r.send_two, r.mid, r.recv_two
    extra_ref, relay_ref, all_ref = r.extra, r.relay, r.extras

    def first(d):
        to = lax.rem(col + d, NC)
        return pltpu.make_async_remote_copy(
            src_ref=send_ref.at[to],
            dst_ref=mid_ref.at[col],
            send_sem=r.send_a.at[0],
            recv_sem=r.recv_a.at[col // PER],
            device_id=(row, to),
            device_id_type=MESH,
        )

    def extra(to):
        return pltpu.make_async_remote_copy(
            src_ref=extra_ref.at[to],
            dst_ref=relay_ref,
            send_sem=r.send_x.at[0],
            recv_sem=r.recv_x.at[0],
            device_id=(row, to),
            device_id_type=MESH,
        )

    def spread_extra(e):
        return pltpu.make_async_remote_copy(
            src_ref=relay_ref,
            dst_ref=all_ref.at[row],
            send_sem=r.send_y.at[0],
            recv_sem=r.recv_y.at[0],
            device_id=(lax.rem(row + e, NR), col),
            device_id_type=MESH,
        )

    def second(g, e):
        to = lax.rem(row + e, NR)
        return pltpu.make_async_remote_copy(
            src_ref=mid_ref.at[pl.ds(g * PER, PER), pl.ds(2 * to, 2)],
            dst_ref=out_ref.at[pl.ds(g * PER, PER), pl.ds(2 * row, 2)],
            send_sem=r.send_b.at[g],
            recv_sem=r.recv_b.at[g],
            device_id=(to, col),
            device_id_type=MESH,
        )

    def keep(g):
        return pltpu.make_async_copy(
            mid_ref.at[pl.ds(g * PER, PER), pl.ds(2 * row, 2)],
            out_ref.at[pl.ds(g * PER, PER), pl.ds(2 * row, 2)],
            r.recv_b.at[g],
        )

    @pl.when(col == 0)
    def _():
        past_end()
        for d in range(1, NC):
            extra(d).start()
        pltpu.make_async_copy(extra_ref.at[0], relay_ref, r.recv_x.at[0]).start()

    for d in ORDER_TWO:
        first(d).start()
    pltpu.make_async_copy(
        send_ref.at[col], mid_ref.at[col], r.recv_a.at[col // PER]
    ).start()
    sets = [lax.rem(col // PER + k, SETS) for k in (0, 1, 3, 2)]
    for i, g in enumerate(sets):
        block = pl.ds(g * PER, PER)
        landed(mid_ref.at[block], send_ref.at[block], r.recv_a.at[g])
        keep(g).start()

        def go(e, carry, g=g):
            second(g, e).start()
            return carry

        lax.fori_loop(1, NR, go, 0)
        if i == 1:
            landed(relay_ref, extra_ref.at[0], r.recv_x.at[0])
            pltpu.make_async_copy(relay_ref, all_ref.at[row], r.recv_y.at[0]).start()

            def go_extra(e, carry):
                spread_extra(e).start()
                return carry

            lax.fori_loop(1, NR, go_extra, 0)
    landed(all_ref, all_ref, r.recv_y.at[0])

    def arrived(i):
        block = pl.ds(sets[i] * PER, PER)
        landed(out_ref.at[block], mid_ref.at[block], r.recv_b.at[sets[i]])
        return sets[i]

    return arrived


def finish(r, col):
    send_ref, mid_ref, across = r.send_two, r.mid, r.across
    most = pl.ds(0, 2 * NC - 1)
    landed(r.recv_one.at[most], r.send_one.at[most], r.send_sem_one.at[0])
    most = pl.ds(0, NC - 1)
    landed(mid_ref.at[most], send_ref.at[most], r.send_a.at[0])

    @pl.when(col == 0)
    def _():
        landed(r.extra.at[most], r.extra.at[most], r.send_x.at[0])

    most = pl.ds(0, NR - 1)
    landed(r.extras.at[most], r.extras.at[most], r.send_y.at[0])
    for g in range(SETS):
        part = (pl.ds(g * PER, PER), pl.ds(0, 2 * NR - 2))
        landed(mid_ref.at[part], send_ref.at[part], r.send_b.at[g])
    whole = (slice(None), pl.ds(0, G))
    landed(across.at[whole], across.at[whole], r.send_h.at[0])


def columns(r, row, arrived):
    in_ref, extra_ref, first_ref, turn_one = r.recv_two, r.extras, r.col_first, r.turn_one
    second_h, second_l, turn_two = r.mix_h, r.mix_l, r.turn_two
    y_h, y_l, middle, z_h, z_l = r.y_h, r.y_l, r.middle, r.z_h, r.z_l
    lane = lax.broadcasted_iota(jnp.int32, (HB, 128), 1)
    held = extra_ref[0:HB, lax.rem(row, 8), :]
    mine = held
    for k in range(1, 4):
        mine = jnp.where(row // 8 == k, pltpu.roll(held, 128 - 32 * k, 1), mine)
    real = jnp.where(lane < 16, mine, 0.0)
    imag = jnp.where(lane < 16, pltpu.roll(mine, 112, 1), 0.0)
    high, low = two_parts(jnp.concatenate([real, imag], axis=0))
    added = dot(first_ref[2], jnp.concatenate([high, high, low], axis=0))
    added = jnp.concatenate([added, jnp.zeros_like(added)], axis=1)

    def two(pair, carry):
        for e in range(2):

            def piece(ri, pair=pair, e=e):
                return jnp.concatenate(
                    [
                        in_ref[pair * 2 + k, pl.ds(e * 32 + ri, HB, stride=2), :]
                        for k in range(2)
                    ],
                    axis=1,
                )

            high, low = two_parts(jnp.concatenate([piece(0), piece(1)], axis=0))
            done = dot(first_ref[e], jnp.concatenate([high, high, low], axis=0))
            if e == 0:
                done = done + jnp.where(pair == 0, added, 0.0)
            cos, sin = turn_one[0], turn_one[1]
            for k in range(2):
                real = done[:NR, k * 128 : (k + 1) * 128]
                imag = done[NR:, k * 128 : (k + 1) * 128]
                high, low = two_parts(
                    jnp.concatenate([real * cos - imag * sin, real * sin + imag * cos], axis=1)
                )
                at = pl.ds(pl.multiple_of(e * 512 + (pair * 2 + k) * NR, NR), NR)
                y_h[at, :] = high
                y_l[at, :] = low
        return carry

    for i in range(SETS):
        g = arrived(i)
        lax.fori_loop(0, PER // 2, lambda k, carry, g=g: two(g * (PER // 2) + k, carry), 0)

    def digits(n, carry):
        at = pl.ds(pl.multiple_of(n * 256, 256), 256)
        middle[:, at] = (
            dot(second_h[...], y_h[at, :], NT)
            + dot(second_l[...], y_h[at, :], NT)
            + dot(second_h[...], y_l[at, :], NT)
        )
        return carry

    lax.fori_loop(0, 4, digits, 0)

    def butterfly(p1, carry):
        at = pl.ds(pl.multiple_of(p1 * 16, 16), 16)
        below = pl.ds(pl.multiple_of(128 + p1 * 16, 16), 16)

        def factor(k):
            return turn_two[k, pl.ds(p1, 1), :]

        real, imag = middle[at, 0:512], middle[below, 0:512]
        other_real, other_imag = middle[at, 512:1024], middle[below, 512:1024]
        cos, sin = factor(0), factor(1)
        other_real, other_imag = (
            other_real * cos - other_imag * sin,
            other_real * sin + other_imag * cos,
        )
        for half in range(2):
            if half == 0:
                one, two_ = real + other_real, imag + other_imag
            else:
                one, two_ = real - other_real, imag - other_imag
            cos, sin = factor(2 + 2 * half), factor(3 + 2 * half)
            high, low = two_parts(
                jnp.concatenate([one * cos - two_ * sin, one * sin + two_ * cos], axis=1)
            )
            to = pl.ds(pl.multiple_of(half * 128 + p1 * 16, 16), 16)
            z_h[to, :] = high
            z_l[to, :] = low
        return carry

    lax.fori_loop(0, 8, butterfly, 0)


def smooth(r, flat, up, down):
    image, third_h, third_l, z_h, z_l = r.image, r.third_h, r.third_l, r.z_h, r.z_l
    own_ref, low_ref, high_ref, taps_ref = r.own, r.low, r.high, r.taps
    across, band_h, band_l, result = r.across, r.band_h, r.band_l, r.out

    def sides(chunk):
        at = pl.ds(chunk * CHUNK, CHUNK)
        return [
            pltpu.make_async_remote_copy(
                own_ref.at[:, at],
                there.at[:, at],
                r.send_h.at[0],
                r.recv_h.at[chunk],
                device_id=peer,
                device_id_type=MESH,
            )
            for i, (there, peer) in enumerate(((low_ref, up), (high_ref, down)))
        ]

    for half in range(2):
        at = slice(half * 256, (half + 1) * 256)
        image[:, at] = (
            dot(z_h[...], third_h[:, at])
            + dot(z_h[...], third_l[:, at])
            + dot(z_l[...], third_h[:, at])
        )
        for p2 in range(half * 8, half * 8 + 8):
            for group in range(4):
                own_ref[:, p2 * 512 + group * 128 : p2 * 512 + (group + 1) * 128] = (
                    jnp.concatenate(
                        [
                            image[
                                (group * 4 + k) * 16 : (group * 4 + k + 1) * 16,
                                p2 * 32 : (p2 + 1) * 32,
                            ]
                            for k in range(4)
                        ],
                        axis=1,
                    )
                )
            if p2 % 4 == 3:
                for copy in sides(p2 // 4):
                    copy.start()

    mix = []
    for m in range(NSCALE):
        distance = lax.broadcasted_iota(jnp.int32, (16, 48), 1) - lax.broadcasted_iota(
            jnp.int32, (16, 48), 0
        )
        v = jnp.zeros((16, 48), F32)
        for t in range(KW):
            v = jnp.where(distance == t, taps_ref[m, t], v)
        mix.append(v)
    mix_h, mix_l = two_parts(jnp.concatenate(mix, axis=0))
    mix = jnp.concatenate([mix_h, mix_l, mix_h], axis=1)
    zero = jnp.zeros((NSCALE * 16, 128), F32)
    across[:, 0:128] = zero
    across[:, 128 + G : 256 + G] = zero
    band_h[...] = jnp.zeros_like(band_h)
    band_l[...] = jnp.zeros_like(band_l)
    difference = lax.broadcasted_iota(jnp.int32, (128, 128), 0) - lax.broadcasted_iota(
        jnp.int32, (128, 128), 1
    )
    for m in range(NSCALE):
        for k in range(3):
            distance = difference + (128 * k - 112)
            v = jnp.zeros((128, 128), F32)
            for t in range(KW):
                v = jnp.where(distance == t, taps_ref[m, t], v)
            high, low = two_parts(v)
            for o in range(2):
                at = slice((k + o) * 128, (k + o + 1) * 128)
                band_h[m, at, o * 128 : (o + 1) * 128] = high
                band_l[m, at, o * 128 : (o + 1) * 128] = low

    no_low, no_high = flat == 0, flat == NR * NC - 1

    def cross(i):
        here = slice(i * 512, (i + 1) * 512)
        below = jnp.where(no_low, 0.0, low_ref[:, here])
        above = jnp.where(no_high, 0.0, high_ref[:, here])
        high, low = two_parts(jnp.concatenate([below, own_ref[:, here], above], axis=0))
        across[:, i * 512 + 128 : i * 512 + 640] = dot(
            mix, jnp.concatenate([high, high, low], axis=0)
        )

    def along(i):
        for m in range(NSCALE):
            window = jnp.concatenate(
                [
                    across[m * 16 : (m + 1) * 16, i * CHUNK + k * 256 : i * CHUNK + k * 256 + 512]
                    for k in range(8)
                ],
                axis=0,
            )
            high, low = two_parts(window)
            done = dot(high, band_h[m]) + dot(low, band_h[m]) + dot(high, band_l[m])
            for k in range(8):
                result[m, :, i * CHUNK + k * 256 : i * CHUNK + (k + 1) * 256] = done[
                    k * 16 : (k + 1) * 16
                ]

    for chunk in range(4):
        landed(across.at[:, 0:CHUNK], across.at[:, 0:CHUNK], r.recv_h.at[chunk])
        for i in range(4):
            cross(chunk * 4 + i)
        if chunk:
            along(chunk - 1)
    along(3)


PRE = "hbm_"
GIVEN = "vis pos w".split() + "tile_v group_v col_v".split()
TABLES = (
    "first turn second_h second_l".split()
    + "col_first turn_one mix_h mix_l".split()
    + "turn_two third_h third_l".split()
)


def per_device(
    vis, vis_pos, vis_w, subgrid_tile, subgrid_group, subgrid_col, grid_kernel, scale_kernels
):
    tile, group = subgrid_tile[:, 0], subgrid_group[:, 0]
    tables = list(row_tables()) + list(column_tables())
    inputs = dict(
        group_s=(SM, group),
        col_s=(SM, subgrid_col),
        grid_taps=(SM, grid_kernel),
        taps=(SM, scale_kernels),
        hbm_vis=(ANY, vis),
        hbm_pos=(ANY, vis_pos),
        hbm_w=(ANY, vis_w.reshape(1, -1)),
        hbm_tile_v=(ANY, tile.reshape(1, -1)),
        hbm_group_v=(ANY, group.reshape(1, -1)),
        hbm_col_v=(ANY, subgrid_col.reshape(1, -1)),
    )
    for name, table in zip(TABLES, tables):
        inputs[PRE + name] = (ANY, jnp.asarray(table))
    dma = pltpu.SemaphoreType.DMA
    scratch = {name: pltpu.VMEM(t.shape, t.dtype) for name, t in zip(TABLES, tables)}
    scratch |= {
        n: pltpu.VMEM(inputs[PRE + n][1].shape, inputs[PRE + n][1].dtype) for n in GIVEN
    }
    scratch |= dict(
        given_sem=dma((len(GIVEN),)),
        table_sem=dma((len(TABLES),)),
        rows=pltpu.VMEM((512, 128), F32),
        send_one=pltpu.VMEM((2 * NC, MSG, 128), F32),
        recv_one=pltpu.VMEM((2 * NC, MSG, 128), F32),
        send_sem_one=dma((1,)),
        recv_sem_one=dma((2, NC)),
        own_sem=dma((1,)),
        u_h=pltpu.VMEM((2048, 256), BF),
        u_l=pltpu.VMEM((2048, 256), BF),
        a_h=pltpu.VMEM((512, 256), BF),
        a_l=pltpu.VMEM((512, 256), BF),
        send_two=pltpu.VMEM((NC, 2 * NR, 128), F32),
        extra=pltpu.VMEM((NC, 8, 128), F32),
        mid=pltpu.VMEM((NC, 2 * NR, 128), F32),
        relay=pltpu.VMEM((8, 128), F32),
        recv_two=pltpu.VMEM((NC, 2 * NR, 128), F32),
        extras=pltpu.VMEM((NR, 8, 128), F32),
        send_a=dma((1,)),
        recv_a=dma((SETS,)),
        send_x=dma((1,)),
        recv_x=dma((1,)),
        send_y=dma((1,)),
        recv_y=dma((1,)),
        send_b=dma((SETS,)),
        recv_b=dma((SETS,)),
        y_h=pltpu.VMEM((1024, 256), BF),
        y_l=pltpu.VMEM((1024, 256), BF),
        middle=pltpu.VMEM((256, 1024), F32),
        z_h=pltpu.VMEM((256, 1024), BF),
        z_l=pltpu.VMEM((256, 1024), BF),
        image=pltpu.VMEM((256, 512), F32),
        own=pltpu.VMEM((16, G), F32),
        low=pltpu.VMEM((16, G), F32),
        high=pltpu.VMEM((16, G), F32),
        send_h=dma((1,)),
        recv_h=dma((4,)),
        across=pltpu.VMEM((NSCALE * 16, G + 256), F32),
        band_h=pltpu.VMEM((NSCALE, 512, 256), BF),
        band_l=pltpu.VMEM((NSCALE, 512, 256), BF),
    )
    names = list(inputs) + ["out"] + list(scratch)
    return pl.pallas_call(
        functools.partial(whole_kernel, names),
        out_shape=pltpu.VMEM((NSCALE, 16, G), F32),
        in_specs=[spec for spec, _ in inputs.values()],
        out_specs=VM,
        scratch_shapes=list(scratch.values()),
        compiler_params=pltpu.CompilerParams(collective_id=0, has_side_effects=True),
        name="whole",
    )(*[value for _, value in inputs.values()])


def solution(mesh):
    return jax.shard_map(
        per_device,
        mesh=mesh,
        in_specs=(
            P(None, ("row", "col")),
            P(None, ("row", "col")),
            P(("row", "col")),
            P(("row", "col"), None),
            P(("row", "col"), None),
            P(("row", "col")),
            P(),
            P(),
        ),
        out_specs=P(None, ("row", "col"), None),
        check_vma=False,
    )
```

```python
import functools
import math
import types

import jax
import jax.numpy as jnp
import ml_dtypes
import numpy as np
from jax import lax
from jax.experimental import pallas as pl
from jax.experimental.pallas import tpu as pltpu
from jax.sharding import PartitionSpec as P

G = 8192
SUB = 32
SUP = 8
OVER = 8
VPS = 256
WSTEPS = 1024
KW = 33
NSCALE = 2
NR = 32
NC = 16
SD = 32
HALO = 16
HB = NR // 2
MSG = SD // 2 + 2

BF = jnp.bfloat16
F32 = jnp.float32
MESH = pl.DeviceIdType.MESH
NN = (((1,), (0,)), ((), ()))
NT = (((1,), (1,)), ((), ()))
VM = pl.BlockSpec(memory_space=pltpu.VMEM)
SM = pl.BlockSpec(memory_space=pltpu.SMEM)
ANY = pl.BlockSpec(memory_space=pl.ANY)


def two_parts(x):
    high = x.astype(BF)
    return high, (x - high.astype(F32)).astype(BF)


def dot(a, b, dims=NN):
    return lax.dot_general(a, b, dims, preferred_element_type=F32)


def np_parts(x):
    x = np.asarray(x, np.float64)
    high = x.astype(np.float32).astype(ml_dtypes.bfloat16)
    low = (x - high.astype(np.float64)).astype(np.float32).astype(ml_dtypes.bfloat16)
    return high, low


def angle_tables(a, b, period):
    turn = 2.0 * math.pi * ((np.asarray(a, np.int64) * np.asarray(b, np.int64)) % period) / period
    return np.cos(turn), np.sin(turn)


def row_tables():
    q0 = np.arange(64)
    cos, sin = angle_tables(q0[:, None], q0[None, :], 64)
    first_h, first_l = np_parts(np.concatenate([cos, sin], 0))
    first = np.concatenate([first_h, first_l, first_h], 1)
    cos, sin = angle_tables(q0[:, None], np.arange(128)[None, :], G)
    twiddle = np.stack([cos, sin]).astype(np.float32)
    high = (4 * np.arange(NR)[None, :] + np.arange(4)[:, None]).reshape(-1)
    cos, sin = angle_tables(high[:, None], np.arange(128)[None, :], 128)
    second = np.concatenate(
        [np.concatenate([cos, -sin], 1), np.concatenate([sin, cos], 1)], 0
    )
    return (first, twiddle, *np_parts(second))


def column_tables():
    p0 = np.arange(NR)

    def first_matrix(bands):
        cos, sin = angle_tables(p0[:, None], bands[None, :], NR)
        high, low = np_parts(np.concatenate([cos, sin], 0))
        return np.concatenate([high, low, high], 1)

    band = np.arange(HB)
    first = np.stack([first_matrix(band), first_matrix(band[::-1]), first_matrix(band + 1)])
    lane = np.arange(128)
    i, ri, jl = lane // 16, (lane // 8) % 2, lane % 8
    cos, sin = angle_tables(p0[:, None], i[None, :], 256)
    turn_one = np.stack([cos, np.where(ri == 1, sin, -sin)]).astype(np.float32)
    d = np.arange(8)
    out_ri, out_p1, out_jl = lane // 64, (lane // 8) % 8, lane % 8
    cos, sin = angle_tables(out_p1[:, None], i[None, :], 8)
    same = out_ri[:, None] == ri[None, :]
    second = np.where(same, cos, np.where(out_ri[:, None] == 1, sin, -sin))
    second = second * (out_jl[:, None] == jl[None, :])
    c, p0s = np.repeat(np.arange(NC), NR)[None, :], np.tile(p0, NC)[None, :]
    part = p0s + NR * d[:, None]
    turns = [angle_tables(part, 1, 512)]
    turns += [angle_tables(c, part + 256 * half, G) for half in range(2)]
    turn_two = np.concatenate([np.stack(t) for t in turns]).astype(np.float32)
    c = np.arange(NC)
    cos, sin = angle_tables(c[:, None], c[None, :], NC)
    eye = np.eye(NR)
    third = np.concatenate([np.kron(cos, eye), -np.kron(sin, eye)], 0) / G
    return (first, turn_one, *np_parts(second), turn_two, *np_parts(third))


ORDER_ONE = [(far, d) for d in (8, 7, 9, 6, 10, 5, 11, 4, 12, 3, 13, 2, 14, 1, 15) for far in (1, 0)]
ORDER_ONE = ORDER_ONE + [(1, 0)]
ORDER_TWO = (1, 15, 2, 14, 3, 13, 4, 12, 5, 11, 6, 10, 7, 9, 8)
SETS = 4
PER = NC // SETS
CHUNK = G // 4


def landed(ref, other, sem):
    pltpu.make_async_copy(other, ref, sem).wait()


def whole_kernel(names, *refs):
    r = types.SimpleNamespace(**dict(zip(names, refs)))
    row, col = lax.axis_index("row"), lax.axis_index("col")
    half = row // HB
    barrier = pltpu.get_barrier_semaphore()
    flat = row * NC + col
    after, before = lax.rem(flat + 1, NR * NC), lax.rem(flat + NR * NC - 1, NR * NC)
    up = (after // NC, lax.rem(after, NC))
    down = (before // NC, lax.rem(before, NC))
    opposite = NR - 1 - row
    peers = [(row, lax.rem(col + d, NC)) for d in range(1, NC)]
    peers += [(opposite, lax.rem(col + d, NC)) for d in range(NC)]
    peers += [(lax.rem(row + e, NR), col) for e in range(1, NR)]
    peers += [up, down]
    given = [
        pltpu.make_async_copy(getattr(r, PRE + n), getattr(r, n), r.given_sem.at[i])
        for i, n in enumerate(GIVEN)
    ]
    for copy in given:
        copy.start()
    for peer in peers:
        pl.semaphore_signal(barrier, inc=1, device_id=peer, device_id_type=MESH)
    tables = [
        pltpu.make_async_copy(getattr(r, PRE + n), getattr(r, n), r.table_sem.at[i])
        for i, n in enumerate(TABLES)
    ]
    for table in tables:
        table.start()
    for copy in given:
        copy.wait()
    gridding(r, half)
    pl.semaphore_wait(barrier, len(peers))
    exchange_one(r, row, col, half, opposite)
    for table in tables:
        table.wait()
    past_end = rows(r, row, col)
    later_stages(r, row, col, past_end, flat, up, down)
    finish(r, col)


def gridding(r, mirror):
    sign = 1 - 2 * mirror
    vis_ref, pos_ref, w_ref, rows_ref, out_ref = r.vis, r.pos, r.w, r.rows, r.send_one
    tap_axis = lax.broadcasted_iota(jnp.int32, (SUP, VPS), 0)
    columns = []
    for t in range(OVER):
        v = jnp.zeros((SUP, VPS), F32)
        for k in range(SUP):
            v = jnp.where(tap_axis == k, r.grid_taps[t, k], v)
        columns.append(v)
    slot = lax.broadcasted_iota(jnp.int32, (SUB, VPS), 0)
    row_axis = jnp.where(
        mirror == 1, jnp.where((slot & 15) == 0, 16 - slot, 32 - slot), slot
    )
    col_axis = slot * sign
    shifted = jnp.where(lax.broadcasted_iota(jnp.int32, (NC, SUB), 0) == 0, mirror, 0)

    def weights(pos):
        step = jnp.broadcast_to(pos & (OVER - 1), (SUP, VPS))
        rows = columns[0]
        for t in range(1, OVER):
            rows = jnp.where(step == t, columns[t], rows)
        return rows

    def spread(rows, distance):
        out = jnp.zeros((SUB, VPS), F32)
        for t in range(SUP):
            out = jnp.where(distance == t, jnp.broadcast_to(rows[t : t + 1, :], (SUB, VPS)), out)
        return out

    def one(s):
        here = pl.ds(pl.multiple_of(s * VPS, VPS), VPS)
        pos_u, pos_v = pos_ref[0:1, here], pos_ref[1:2, here]
        angle = w_ref[0:1, here].astype(F32) * (2.0 * math.pi / WSTEPS)
        cosine, sine = jnp.cos(angle), jnp.sin(angle)
        real, imag = vis_ref[0:1, here], vis_ref[1:2, here]
        turned_real = real * cosine + imag * sine
        turned_imag = (imag * cosine - real * sine) * sign.astype(F32)
        along_u = spread(weights(pos_u), row_axis - lax.shift_right_logical(pos_u, 3))
        corner = r.col_s[s] & (SUB - 1)
        corner = jnp.where(mirror == 1, 1 - corner, corner) & (SUB - 1)
        start = (31 * mirror - sign * corner) - lax.shift_right_logical(pos_v, 3)
        along_v = spread(weights(pos_v), (col_axis + start) & (SUB - 1))
        left_h, left_l = two_parts(
            jnp.concatenate([along_u * turned_real, along_u * turned_imag], axis=0)
        )
        right_h, right_l = two_parts(along_v)
        block = dot(left_h, right_h, NT) + dot(left_l, right_h, NT) + dot(left_h, right_l, NT)
        odd = ((shifted + r.group_s[s]) & 1) == 1
        even_rows, odd_rows = [], []
        for ri in range(2):
            near, far = block[ri * 32 : ri * 32 + 16], block[ri * 32 + 16 : ri * 32 + 32]
            even_rows.append(jnp.where(odd, far, near))
            odd_rows.append(jnp.where(odd, near, far))
        return even_rows, odd_rows

    def pair(s, carry):
        here, there = one(s), one(s + SD // 2)
        for e in range(2):
            rows_ref[pl.ds(e * 256 + s, NC, stride=SD // 2), :] = jnp.concatenate(
                here[e] + there[e], axis=1
            )
        return carry

    lax.fori_loop(0, SD // 2, pair, 0)
    l0 = r.tile_v[...] * (G // NC) + r.col_v[...]
    l0 = jnp.where(mirror == 1, G - SUB + 1 - l0, l0).astype(F32)
    group = jnp.where(mirror == 1, 14 - r.group_v[...], r.group_v[...]).astype(F32)
    meta = jnp.concatenate(
        [jnp.concatenate([l0] * 4, axis=1), jnp.concatenate([group] * 4, axis=1)], axis=0
    )
    lane = lax.broadcasted_iota(jnp.int32, (2, 128), 1)
    mine = lax.shift_right_logical(lane, 5) == lax.rem(lax.axis_index("col"), 4)
    meta = jnp.where(mine, meta, 0.0)
    for k in range(2 * NC):
        out_ref[k, 0:16, :] = rows_ref[k * 16 : (k + 1) * 16, :]
        out_ref[k, 16:18, :] = meta


def unpack(r, z):
    recv_ref, u_h, u_l = r.recv_one, r.u_h, r.u_l
    lane = lax.broadcasted_iota(jnp.int32, (SD, 128), 1)
    sub = lax.broadcasted_iota(jnp.int32, (SD, 128), 0)
    segment = lax.shift_right_logical(lane[0:16], 5)
    data = recv_ref[z, 0:16, :]
    corner = recv_ref[z, 16:17, :]
    mine = lane == sub + SD * (z & 3)
    l0 = jnp.sum(
        jnp.where(mine, jnp.broadcast_to(corner, (SD, 128)), 0.0), axis=1, keepdims=True
    )
    distance = lane - (l0.astype(jnp.int32) & 127)
    rolled = [data] + [pltpu.roll(data, SUB * k, 1) for k in range(1, 4)]
    wide = []
    for i in range(4):
        v = rolled[(0 - i) % 4]
        for p in range(1, 4):
            v = jnp.where(segment == p, rolled[(p - i) % 4], v)
        wide.append(v)
    real = jnp.concatenate([wide[0], wide[2]], axis=0)
    imag = jnp.concatenate([wide[1], wide[3]], axis=0)
    in_a = (distance >= 0) & (distance < SUB)
    in_b = distance < SUB - 128
    for ab, inside in enumerate((in_a, in_b)):
        high, low = two_parts(
            jnp.concatenate(
                [jnp.where(inside, real, 0.0), jnp.where(inside, imag, 0.0)], axis=1
            )
        )
        at = pl.ds(pl.multiple_of(ab * 1024 + z * SD, SD), SD)
        u_h[at, :] = high
        u_l[at, :] = low


def exchange_one(r, row, col, half, opposite):
    send_ref, recv_ref = r.send_one, r.recv_one

    def copy(far, d):
        to = lax.rem(col + d, NC)
        there = half + far * (1 - 2 * half)
        return pltpu.make_async_remote_copy(
            src_ref=send_ref.at[there * NC + to],
            dst_ref=recv_ref.at[half * NC + col],
            send_sem=r.send_sem_one.at[0],
            recv_sem=r.recv_sem_one.at[far, d],
            device_id=(row + far * (opposite - row), to),
            device_id_type=MESH,
        )

    for far, d in ORDER_ONE:
        copy(far, d).start()
    own = pltpu.make_async_copy(
        send_ref.at[half * NC + col], recv_ref.at[half * NC + col], r.own_sem.at[0]
    )
    own.start()
    own.wait()
    unpack(r, half * NC + col)

    def arrive(i, carry):
        step = i // 2
        far = 1 - lax.rem(i, 2)
        d = 8 + ((step + 1) // 2) * (1 - 2 * lax.rem(step, 2))
        copy(far, d).wait_recv()
        there = half + far * (1 - 2 * half)
        unpack(r, there * NC + lax.rem(col + NC - d, NC))
        return carry

    lax.fori_loop(0, 2 * NC - 1, arrive, 0)


def rows(r, row, col):
    recv_ref, first_ref, turn_ref = r.recv_one, r.first, r.turn
    second_h, second_l, out_ref, extra_ref = r.second_h, r.second_l, r.send_two, r.extra
    u_h, u_l, a_h, a_l = r.u_h, r.u_l, r.a_h, r.a_l
    parity = row // HB
    shifted = jnp.where(col == 0, 1, 0)
    index = []
    for group in range(8):
        corner = sum(recv_ref[group * 4 + i, 16:17, :] for i in range(4)).astype(jnp.int32)
        start = sum(recv_ref[group * 4 + i, 17:18, :] for i in range(4)).astype(jnp.int32)
        if group >= 4:
            start = start + shifted
        start = lax.shift_right_logical(start + ((start ^ parity) & 1), 1) * 64
        tile = lax.shift_right_logical(corner, 7)
        index.append((start + tile, start + ((tile + 1) & 63)))
    chunks = [
        jnp.concatenate([index[k][ab], index[k + 1][ab]], axis=1)
        for ab in range(2)
        for k in range(0, 8, 2)
    ]

    def placed(first, count):
        place = lax.broadcasted_iota(jnp.int32, (count, 256), 0) + first
        total = jnp.zeros((count, 256), F32)
        for k in range(8):
            pick = (place == chunks[k]).astype(F32).astype(BF)
            at = slice(k * 256, (k + 1) * 256)
            total = total + dot(pick, u_h[at, :]) + dot(pick, u_l[at, :])
        return total

    def inner(value):
        high, low = two_parts(value)
        both = dot(first_ref[...], jnp.concatenate([high, high, low], axis=0))
        real = both[:64, :128] - both[64:, 128:]
        imag = both[64:, :128] + both[:64, 128:]
        cos, sin = turn_ref[0], turn_ref[1]
        return two_parts(
            jnp.concatenate([real * cos - imag * sin, real * sin + imag * cos], axis=1)
        )

    def outer(high, low):
        return (
            dot(second_h[...], high, NT) + dot(second_l[...], high, NT) + dot(second_h[...], low, NT)
        )

    def four_rows(block, carry):
        total = placed(block * 256, 256)
        for k in range(4):
            high, low = inner(total[k * 64 : (k + 1) * 64])
            for cl in range(4):
                at = pl.ds(pl.multiple_of(cl * 128 + (block * 4 + k) * 16, 16), 16)
                a_h[at, :] = high[cl * 16 : (cl + 1) * 16]
                a_l[at, :] = low[cl * 16 : (cl + 1) * 16]
        return carry

    lax.fori_loop(0, 2, four_rows, 0)
    for pair in range(2):
        at = slice(pair * 256, (pair + 1) * 256)
        done = outer(a_h[at, :], a_l[at, :])
        for ch in range(4):
            for k in range(2):
                at = slice(ch * 32, (ch + 1) * 32)
                real = done[:128][at, k * 128 : (k + 1) * 128]
                imag = done[128:][at, k * 128 : (k + 1) * 128]
                upper = (lax.broadcasted_iota(jnp.int32, (NR, 128), 1) & 8) != 0
                to = 4 * ch + 2 * pair + k
                out_ref[0, to] = jnp.where(upper, pltpu.roll(imag, 8, 1), real)
                out_ref[1, to] = jnp.where(upper, imag, pltpu.roll(real, 120, 1))

    def past_end():
        high, low = inner(placed(512, 64))
        done = outer(high, low)
        done = jnp.concatenate([done, jnp.zeros((256, 64), F32)], axis=1)
        where = lax.broadcasted_iota(jnp.int32, (8, 128), 1)
        where = lax.shift_right_logical(where, 4)
        for ch in range(4):
            for cl in range(4):
                v = jnp.zeros((8, 128), F32)
                for ri in range(2):
                    for part in range(4):
                        r0 = ri * 128 + ch * 32 + part * 8
                        to = part * 2 + ri
                        moved = pltpu.roll(done[r0 : r0 + 8], ((to - cl) * 16) % 128, 1)
                        v = jnp.where(where == to, moved, v)
                extra_ref[4 * ch + cl] = v

    return past_end


def swapped(x):
    upper = (lax.broadcasted_iota(jnp.int32, x.shape, 1) & 8) != 0
    return jnp.where(upper, pltpu.roll(x, 8, 1), pltpu.roll(x, 120, 1))


def joined(both):
    upper = (lax.broadcasted_iota(jnp.int32, (NR, 128), 1) & 8) != 0
    turned = swapped(both[NR:])
    return both[:NR] + jnp.where(upper, turned, -turned)


def later_stages(r, row, col, past_end, flat, up, down):
    send_ref, mid_ref, in_ref = r.send_two, r.mid, r.recv_two
    extra_ref, relay_ref, all_ref = r.extra, r.relay, r.extras
    sets = [lax.rem(col // PER + k, SETS) for k in (0, 1, 3, 2)]

    def first(part, d):
        to = lax.rem(col + d, NC)
        return pltpu.make_async_remote_copy(
            src_ref=send_ref.at[part, to],
            dst_ref=mid_ref.at[part, col],
            send_sem=r.send_a.at[0],
            recv_sem=r.recv_a.at[part * SETS + col // PER],
            device_id=(row, to),
            device_id_type=MESH,
        )

    def extra(to):
        return pltpu.make_async_remote_copy(
            src_ref=extra_ref.at[to],
            dst_ref=relay_ref,
            send_sem=r.send_x.at[0],
            recv_sem=r.recv_x.at[0],
            device_id=(row, to),
            device_id_type=MESH,
        )

    def spread_extra(e):
        return pltpu.make_async_remote_copy(
            src_ref=relay_ref,
            dst_ref=all_ref.at[row],
            send_sem=r.send_y.at[0],
            recv_sem=r.recv_y.at[0],
            device_id=(lax.rem(row + e, NR), col),
            device_id_type=MESH,
        )

    def second(part, g, e):
        to = lax.rem(row + e, NR)
        return pltpu.make_async_remote_copy(
            src_ref=mid_ref.at[part, pl.ds(g * PER, PER), pl.ds(to, 1)],
            dst_ref=in_ref.at[part, pl.ds(g * PER, PER), pl.ds(row, 1)],
            send_sem=r.send_b.at[0],
            recv_sem=r.recv_b.at[part * SETS + g],
            device_id=(to, col),
            device_id_type=MESH,
        )

    def relay(part, i):
        g = sets[i]
        block = pl.ds(g * PER, PER)
        landed(mid_ref.at[part, block], send_ref.at[part, block], r.recv_a.at[part * SETS + g])
        pltpu.make_async_copy(
            mid_ref.at[part, block, pl.ds(row, 1)],
            in_ref.at[part, block, pl.ds(row, 1)],
            r.recv_b.at[part * SETS + g],
        ).start()

        def go(e, carry):
            second(part, g, e).start()
            return carry

        lax.fori_loop(1, NR, go, 0)

    @pl.when(col == 0)
    def _():
        past_end()
        for d in range(1, NC):
            extra(d).start()
        pltpu.make_async_copy(extra_ref.at[0], relay_ref, r.recv_x.at[0]).start()

    for part in range(2):
        for d in ORDER_TWO:
            first(part, d).start()
        pltpu.make_async_copy(
            send_ref.at[part, col],
            mid_ref.at[part, col],
            r.recv_a.at[part * SETS + col // PER],
        ).start()

    relay(0, 0)
    relay(0, 1)
    landed(relay_ref, extra_ref.at[0], r.recv_x.at[0])
    pltpu.make_async_copy(relay_ref, all_ref.at[row], r.recv_y.at[0]).start()

    def go_extra(e, carry):
        spread_extra(e).start()
        return carry

    lax.fori_loop(1, NR, go_extra, 0)
    relay(0, 2)
    relay(0, 3)
    bands(r)
    relay(1, 0)
    first_digit(r, row, sets, 0)
    relay(1, 1)
    other_digits(r, 0)
    last_digit(r, 0, up, down)
    relay(1, 2)
    relay(1, 3)
    first_digit(r, row, sets, 1)
    other_digits(r, 1)
    last_digit(r, 1, up, down)
    smooth(r, flat)


def finish(r, col):
    send_ref, mid_ref, across = r.send_two, r.mid, r.across
    most = pl.ds(0, 2 * NC - 1)
    landed(r.recv_one.at[most], r.send_one.at[most], r.send_sem_one.at[0])
    most = pl.ds(0, NC - 1)
    landed(mid_ref.at[:, most], send_ref.at[:, most], r.send_a.at[0])

    @pl.when(col == 0)
    def _():
        landed(r.extra.at[most], r.extra.at[most], r.send_x.at[0])

    most = pl.ds(0, NR - 1)
    landed(r.extras.at[most], r.extras.at[most], r.send_y.at[0])
    landed(mid_ref.at[:, :, most], send_ref.at[:, :, most], r.send_b.at[0])
    landed(across.at[:, 0:G], across.at[:, 0:G], r.send_h.at[0])


def first_digit(r, row, sets, part):
    in_ref, first_ref, turn_one = r.recv_two, r.col_first, r.turn_one
    if part == 0:
        landed(r.extras, r.extras, r.recv_y.at[0])
    lane = lax.broadcasted_iota(jnp.int32, (HB, 128), 1)
    held = r.extras[0:HB, lax.rem(row, 8), :]
    mine = held
    for k in range(1, 4):
        mine = jnp.where(row // 8 == k, pltpu.roll(held, 128 - 32 * k, 1), mine)
    near = mine if part == 0 else pltpu.roll(mine, 120, 1)
    far = pltpu.roll(mine, 120 - 8 * part, 1)
    high, low = two_parts(jnp.where(lane < 8, near, jnp.where(lane < 16, far, 0.0)))
    added = joined(dot(first_ref[2], jnp.concatenate([high, high, low], axis=0)))

    def two(pair):
        for e in range(2):
            value = jnp.concatenate(
                [in_ref[part, pair * 2 + k, e * HB : (e + 1) * HB, :] for k in range(2)], axis=1
            )
            high, low = two_parts(value)
            done = dot(first_ref[e], jnp.concatenate([high, high, low], axis=0))
            for k in range(2):
                value = joined(done[:, k * 128 : (k + 1) * 128])
                if e == 0 and k == 0:
                    value = value + jnp.where(pair == 0, added, 0.0)
                high, low = two_parts(value * turn_one[0] + swapped(value) * turn_one[1])
                at = pl.ds(pl.multiple_of(e * 512 + (pair * 2 + k) * NR, NR), NR)
                r.y_h[at, :] = high
                r.y_l[at, :] = low

    for i in range(SETS):
        g = sets[i]
        block = pl.ds(g * PER, PER)
        landed(in_ref.at[part, block], r.mid.at[part, block], r.recv_b.at[part * SETS + g])

        def step(k, carry, g=g):
            two(g * (PER // 2) + k)
            return carry

        lax.fori_loop(0, PER // 2, step, 0)


def other_digits(r, part):
    second_h, second_l, turn_two, middle = r.mix_h, r.mix_l, r.turn_two, r.middle

    def digits(n, carry):
        at = pl.ds(pl.multiple_of(n * 256, 256), 256)
        middle[:, at] = (
            dot(second_h[...], r.y_h[at, :], NT)
            + dot(second_l[...], r.y_h[at, :], NT)
            + dot(second_h[...], r.y_l[at, :], NT)
        )
        return carry

    lax.fori_loop(0, 4, digits, 0)

    def butterfly(k, carry):
        at = pl.ds(pl.multiple_of(k * 16, 16), 16)
        below = pl.ds(pl.multiple_of(64 + k * 16, 16), 16)

        def factor(n):
            return jnp.concatenate(
                [
                    jnp.broadcast_to(turn_two[n, pl.ds(2 * k + j, 1), :], (8, 512))
                    for j in range(2)
                ],
                axis=0,
            )

        real, imag = middle[at, 0:512], middle[below, 0:512]
        other_real, other_imag = middle[at, 512:1024], middle[below, 512:1024]
        cos, sin = factor(0), factor(1)
        other_real, other_imag = (
            other_real * cos - other_imag * sin,
            other_real * sin + other_imag * cos,
        )
        for half in range(2):
            if half == 0:
                one, two = real + other_real, imag + other_imag
            else:
                one, two = real - other_real, imag - other_imag
            cos, sin = factor(2 + 2 * half), factor(3 + 2 * half)
            high, low = two_parts(
                jnp.concatenate([one * cos - two * sin, one * sin + two * cos], axis=1)
            )
            to = pl.ds(pl.multiple_of(half * 64 + k * 16, 16), 16)
            r.z_h[to, :] = high
            r.z_l[to, :] = low
        return carry

    lax.fori_loop(0, 4, butterfly, 0)


def last_digit(r, part, up, down):
    image, third_h, third_l, z_h, z_l, own_ref = r.image, r.third_h, r.third_l, r.z_h, r.z_l, r.own
    rows = pl.ds(part * 8, 8)

    def sides(at, sem):
        return [
            pltpu.make_async_remote_copy(
                own_ref.at[rows, at],
                there.at[rows, at],
                r.send_h.at[0],
                r.recv_h.at[sem],
                device_id=peer,
                device_id_type=MESH,
            )
            for there, peer in ((r.low, up), (r.high, down))
        ]

    for half in range(2):
        at = slice(half * 256, (half + 1) * 256)
        image[:, at] = (
            dot(z_h[...], third_h[:, at])
            + dot(z_h[...], third_l[:, at])
            + dot(z_l[...], third_h[:, at])
        )
        for p2 in range(half * 8, half * 8 + 8):
            for group in range(4):
                own_ref[rows, p2 * 512 + group * 128 : p2 * 512 + (group + 1) * 128] = (
                    jnp.concatenate(
                        [
                            image[
                                (group * 4 + k) * 8 : (group * 4 + k + 1) * 8,
                                p2 * 32 : (p2 + 1) * 32,
                            ]
                            for k in range(4)
                        ],
                        axis=1,
                    )
                )
            if part == 1 and p2 % 4 == 3:
                for copy in sides(pl.ds(p2 // 4 * CHUNK, CHUNK), 1 + p2 // 4):
                    copy.start()
    if part == 0:
        for copy in sides(pl.ds(0, G), 0):
            copy.start()


def bands(r):
    taps_ref, across, band_h, band_l = r.taps, r.across, r.band_h, r.band_l
    mix = []
    for m in range(NSCALE):
        distance = lax.broadcasted_iota(jnp.int32, (16, 48), 1) - lax.broadcasted_iota(
            jnp.int32, (16, 48), 0
        )
        v = jnp.zeros((16, 48), F32)
        for t in range(KW):
            v = jnp.where(distance == t, taps_ref[m, t], v)
        mix.append(v)
    mix_h, mix_l = two_parts(jnp.concatenate(mix, axis=0))
    r.cross_mix[...] = jnp.concatenate([mix_h, mix_l, mix_h], axis=1)
    zero = jnp.zeros((NSCALE * 16, 128), F32)
    across[:, 0:128] = zero
    across[:, 128 + G : 256 + G] = zero
    band_h[...] = jnp.zeros_like(band_h)
    band_l[...] = jnp.zeros_like(band_l)
    difference = lax.broadcasted_iota(jnp.int32, (128, 128), 0) - lax.broadcasted_iota(
        jnp.int32, (128, 128), 1
    )
    for m in range(NSCALE):
        for k in range(3):
            distance = difference + (128 * k - 112)
            v = jnp.zeros((128, 128), F32)
            for t in range(KW):
                v = jnp.where(distance == t, taps_ref[m, t], v)
            high, low = two_parts(v)
            for o in range(2):
                at = slice((k + o) * 128, (k + o + 1) * 128)
                band_h[m, at, o * 128 : (o + 1) * 128] = high
                band_l[m, at, o * 128 : (o + 1) * 128] = low


def smooth(r, flat):
    own_ref, low_ref, high_ref = r.own, r.low, r.high
    across, band_h, band_l, result = r.across, r.band_h, r.band_l, r.out
    no_low, no_high = flat == 0, flat == NR * NC - 1

    def cross(i):
        here = slice(i * 512, (i + 1) * 512)
        below = jnp.where(no_low, 0.0, low_ref[:, here])
        above = jnp.where(no_high, 0.0, high_ref[:, here])
        high, low = two_parts(jnp.concatenate([below, own_ref[:, here], above], axis=0))
        across[:, i * 512 + 128 : i * 512 + 640] = dot(
            r.cross_mix[...], jnp.concatenate([high, high, low], axis=0)
        )

    def along(i):
        for m in range(NSCALE):
            window = jnp.concatenate(
                [
                    across[m * 16 : (m + 1) * 16, i * CHUNK + k * 256 : i * CHUNK + k * 256 + 512]
                    for k in range(8)
                ],
                axis=0,
            )
            high, low = two_parts(window)
            done = dot(high, band_h[m]) + dot(low, band_h[m]) + dot(high, band_l[m])
            for k in range(8):
                result[m, :, i * CHUNK + k * 256 : i * CHUNK + (k + 1) * 256] = done[
                    k * 16 : (k + 1) * 16
                ]

    landed(across.at[0:16, 0:G], across.at[0:16, 0:G], r.recv_h.at[0])
    for chunk in range(4):
        landed(across.at[0:16, 0:CHUNK], across.at[0:16, 0:CHUNK], r.recv_h.at[1 + chunk])
        for i in range(4):
            cross(chunk * 4 + i)
        if chunk:
            along(chunk - 1)
    along(3)


PRE = "hbm_"
GIVEN = "vis pos w".split() + "tile_v group_v col_v".split()
TABLES = (
    "first turn second_h second_l".split()
    + "col_first turn_one mix_h mix_l".split()
    + "turn_two third_h third_l".split()
)


def per_device(
    vis, vis_pos, vis_w, subgrid_tile, subgrid_group, subgrid_col, grid_kernel, scale_kernels
):
    tile, group = subgrid_tile[:, 0], subgrid_group[:, 0]
    tables = list(row_tables()) + list(column_tables())
    inputs = dict(
        group_s=(SM, group),
        col_s=(SM, subgrid_col),
        grid_taps=(SM, grid_kernel),
        taps=(SM, scale_kernels),
        hbm_vis=(ANY, vis),
        hbm_pos=(ANY, vis_pos),
        hbm_w=(ANY, vis_w.reshape(1, -1)),
        hbm_tile_v=(ANY, tile.reshape(1, -1)),
        hbm_group_v=(ANY, group.reshape(1, -1)),
        hbm_col_v=(ANY, subgrid_col.reshape(1, -1)),
    )
    for name, table in zip(TABLES, tables):
        inputs[PRE + name] = (ANY, jnp.asarray(table))
    dma = pltpu.SemaphoreType.DMA
    scratch = {name: pltpu.VMEM(t.shape, t.dtype) for name, t in zip(TABLES, tables)}
    scratch |= {
        n: pltpu.VMEM(inputs[PRE + n][1].shape, inputs[PRE + n][1].dtype) for n in GIVEN
    }
    scratch |= dict(
        given_sem=dma((len(GIVEN),)),
        table_sem=dma((len(TABLES),)),
        rows=pltpu.VMEM((512, 128), F32),
        send_one=pltpu.VMEM((2 * NC, MSG, 128), F32),
        recv_one=pltpu.VMEM((2 * NC, MSG, 128), F32),
        send_sem_one=dma((1,)),
        recv_sem_one=dma((2, NC)),
        own_sem=dma((1,)),
        u_h=pltpu.VMEM((2048, 256), BF),
        u_l=pltpu.VMEM((2048, 256), BF),
        a_h=pltpu.VMEM((512, 256), BF),
        a_l=pltpu.VMEM((512, 256), BF),
        send_two=pltpu.VMEM((2, NC, NR, 128), F32),
        extra=pltpu.VMEM((NC, 8, 128), F32),
        mid=pltpu.VMEM((2, NC, NR, 128), F32),
        relay=pltpu.VMEM((8, 128), F32),
        recv_two=pltpu.VMEM((2, NC, NR, 128), F32),
        extras=pltpu.VMEM((NR, 8, 128), F32),
        send_a=dma((1,)),
        recv_a=dma((2 * SETS,)),
        send_x=dma((1,)),
        recv_x=dma((1,)),
        send_y=dma((1,)),
        recv_y=dma((1,)),
        send_b=dma((1,)),
        recv_b=dma((2 * SETS,)),
        y_h=pltpu.VMEM((1024, 128), BF),
        y_l=pltpu.VMEM((1024, 128), BF),
        middle=pltpu.VMEM((128, 1024), F32),
        z_h=pltpu.VMEM((128, 1024), BF),
        z_l=pltpu.VMEM((128, 1024), BF),
        image=pltpu.VMEM((128, 512), F32),
        cross_mix=pltpu.VMEM((NSCALE * 16, 144), BF),
        own=pltpu.VMEM((16, G), F32),
        low=pltpu.VMEM((16, G), F32),
        high=pltpu.VMEM((16, G), F32),
        send_h=dma((1,)),
        recv_h=dma((5,)),
        across=pltpu.VMEM((NSCALE * 16, G + 256), F32),
        band_h=pltpu.VMEM((NSCALE, 512, 256), BF),
        band_l=pltpu.VMEM((NSCALE, 512, 256), BF),
    )
    names = list(inputs) + ["out"] + list(scratch)
    return pl.pallas_call(
        functools.partial(whole_kernel, names),
        out_shape=pltpu.VMEM((NSCALE, 16, G), F32),
        in_specs=[spec for spec, _ in inputs.values()],
        out_specs=VM,
        scratch_shapes=list(scratch.values()),
        compiler_params=pltpu.CompilerParams(collective_id=0, has_side_effects=True),
        name="whole",
    )(*[value for _, value in inputs.values()])


def solution(mesh):
    return jax.shard_map(
        per_device,
        mesh=mesh,
        in_specs=(
            P(None, ("row", "col")),
            P(None, ("row", "col")),
            P(("row", "col")),
            P(("row", "col"), None),
            P(("row", "col"), None),
            P(("row", "col")),
            P(),
            P(),
        ),
        out_specs=P(None, ("row", "col"), None),
        check_vma=False,
    )
```

```python
import functools
import math
import types

import jax
import jax.numpy as jnp
import ml_dtypes
import numpy as np
from jax import lax
from jax.experimental import pallas as pl
from jax.experimental.pallas import tpu as pltpu
from jax.sharding import PartitionSpec as P

G = 8192
SUB = 32
SUP = 8
OVER = 8
VPS = 256
WSTEPS = 1024
KW = 33
NSCALE = 2
NR = 32
NC = 16
SD = 32
HALO = 16
HB = NR // 2
MSG = SD // 2 + 2

BF = jnp.bfloat16
F32 = jnp.float32
MESH = pl.DeviceIdType.MESH
NN = (((1,), (0,)), ((), ()))
NT = (((1,), (1,)), ((), ()))
VM = pl.BlockSpec(memory_space=pltpu.VMEM)
SM = pl.BlockSpec(memory_space=pltpu.SMEM)
ANY = pl.BlockSpec(memory_space=pl.ANY)


def two_parts(x):
    high = x.astype(BF)
    return high, (x - high.astype(F32)).astype(BF)


def dot(a, b, dims=NN):
    return lax.dot_general(a, b, dims, preferred_element_type=F32)


def np_parts(x):
    x = np.asarray(x, np.float64)
    high = x.astype(np.float32).astype(ml_dtypes.bfloat16)
    low = (x - high.astype(np.float64)).astype(np.float32).astype(ml_dtypes.bfloat16)
    return high, low


def angle_tables(a, b, period):
    turn = 2.0 * math.pi * ((np.asarray(a, np.int64) * np.asarray(b, np.int64)) % period) / period
    return np.cos(turn), np.sin(turn)


def row_tables():
    q0 = np.arange(64)
    cos, sin = angle_tables(q0[:, None], q0[None, :], 64)
    first_h, first_l = np_parts(np.concatenate([cos, sin], 0))
    first = np.concatenate([first_h, first_l, first_h], 1)
    cos, sin = angle_tables(q0[:, None], np.arange(128)[None, :], G)
    twiddle = np.stack([cos, sin]).astype(np.float32)
    high = (4 * np.arange(NR)[None, :] + np.arange(4)[:, None]).reshape(-1)
    cos, sin = angle_tables(high[:, None], np.arange(128)[None, :], 128)
    second = np.concatenate(
        [np.concatenate([cos, -sin], 1), np.concatenate([sin, cos], 1)], 0
    )
    return (first, twiddle, *np_parts(second))


def column_tables():
    p0 = np.arange(NR)

    def first_matrix(bands):
        cos, sin = angle_tables(p0[:, None], bands[None, :], NR)
        high, low = np_parts(np.concatenate([cos, sin], 0))
        return np.concatenate([high, low, high], 1)

    band = np.arange(HB)
    first = np.stack([first_matrix(band), first_matrix(band[::-1]), first_matrix(band + 1)])
    lane = np.arange(128)
    i, ri, jl = lane // 16, (lane // 8) % 2, lane % 8
    cos, sin = angle_tables(p0[:, None], i[None, :], 256)
    turn_one = np.stack([cos, np.where(ri == 1, sin, -sin)]).astype(np.float32)
    d = np.arange(8)
    out_ri, out_p1, out_jl = lane // 64, (lane // 8) % 8, lane % 8
    cos, sin = angle_tables(out_p1[:, None], i[None, :], 8)
    same = out_ri[:, None] == ri[None, :]
    second = np.where(same, cos, np.where(out_ri[:, None] == 1, sin, -sin))
    second = second * (out_jl[:, None] == jl[None, :])
    c, p0s = np.repeat(np.arange(NC), NR)[None, :], np.tile(p0, NC)[None, :]
    part = p0s + NR * d[:, None]
    turns = [angle_tables(part, 1, 512)]
    turns += [angle_tables(c, part + 256 * half, G) for half in range(2)]
    turn_two = np.concatenate([np.stack(t) for t in turns]).astype(np.float32)
    c = np.arange(NC)
    cos, sin = angle_tables(c[:, None], c[None, :], NC)
    eye = np.eye(NR)
    third = np.concatenate([np.kron(cos, eye), -np.kron(sin, eye)], 0) / G
    return (first, turn_one, *np_parts(second), turn_two, *np_parts(third))


ORDER_ONE = [(far, d) for d in (8, 7, 9, 6, 10, 5, 11, 4, 12, 3, 13, 2, 14, 1, 15) for far in (1, 0)]
ORDER_ONE = ORDER_ONE + [(1, 0)]
ORDER_TWO = (1, 15, 2, 14, 3, 13, 4, 12, 5, 11, 6, 10, 7, 9, 8)
SETS = 4
PER = NC // SETS
CHUNK = G // 4


def landed(ref, other, sem):
    pltpu.make_async_copy(other, ref, sem).wait()


def whole_kernel(names, *refs):
    r = types.SimpleNamespace(**dict(zip(names, refs)))
    row, col = lax.axis_index("row"), lax.axis_index("col")
    half = row // HB
    barrier = pltpu.get_barrier_semaphore()
    flat = row * NC + col
    after, before = lax.rem(flat + 1, NR * NC), lax.rem(flat + NR * NC - 1, NR * NC)
    up = (after // NC, lax.rem(after, NC))
    down = (before // NC, lax.rem(before, NC))
    opposite = NR - 1 - row
    peers = [(row, lax.rem(col + d, NC)) for d in range(1, NC)]
    peers += [(opposite, lax.rem(col + d, NC)) for d in range(NC)]
    peers += [(lax.rem(row + e, NR), col) for e in range(1, NR)]
    peers += [up, down]
    given = [
        pltpu.make_async_copy(getattr(r, PRE + n), getattr(r, n), r.given_sem.at[i])
        for i, n in enumerate(GIVEN)
    ]
    for copy in given:
        copy.start()
    for peer in peers:
        pl.semaphore_signal(barrier, inc=1, device_id=peer, device_id_type=MESH)
    tables = [
        pltpu.make_async_copy(getattr(r, PRE + n), getattr(r, n), r.table_sem.at[i])
        for i, n in enumerate(TABLES)
    ]
    for table in tables:
        table.start()
    for copy in given:
        copy.wait()
    gridding(r, half)
    pl.semaphore_wait(barrier, len(peers))
    exchange_one(r, row, col, half, opposite)
    for table in tables:
        table.wait()
    past_end = rows(r, row, col)
    later_stages(r, row, col, past_end, flat, up, down)
    finish(r, col)


def gridding(r, mirror):
    sign = 1 - 2 * mirror
    vis_ref, pos_ref, w_ref, rows_ref, out_ref = r.vis, r.pos, r.w, r.rows, r.send_one
    tap_axis = lax.broadcasted_iota(jnp.int32, (SUP, VPS), 0)
    columns = []
    for t in range(OVER):
        v = jnp.zeros((SUP, VPS), F32)
        for k in range(SUP):
            v = jnp.where(tap_axis == k, r.grid_taps[t, k], v)
        columns.append(v)
    slot = lax.broadcasted_iota(jnp.int32, (SUB, VPS), 0)
    row_axis = jnp.where(
        mirror == 1, jnp.where((slot & 15) == 0, 16 - slot, 32 - slot), slot
    )
    col_axis = slot * sign
    shifted = jnp.where(lax.broadcasted_iota(jnp.int32, (NC, SUB), 0) == 0, mirror, 0)

    def weights(pos):
        step = jnp.broadcast_to(pos & (OVER - 1), (SUP, VPS))
        rows = columns[0]
        for t in range(1, OVER):
            rows = jnp.where(step == t, columns[t], rows)
        return rows

    def spread(rows, distance):
        out = jnp.zeros((SUB, VPS), F32)
        for t in range(SUP):
            out = jnp.where(distance == t, jnp.broadcast_to(rows[t : t + 1, :], (SUB, VPS)), out)
        return out

    def one(s):
        here = pl.ds(pl.multiple_of(s * VPS, VPS), VPS)
        pos_u, pos_v = pos_ref[0:1, here], pos_ref[1:2, here]
        angle = w_ref[0:1, here].astype(F32) * (2.0 * math.pi / WSTEPS)
        cosine, sine = jnp.cos(angle), jnp.sin(angle)
        real, imag = vis_ref[0:1, here], vis_ref[1:2, here]
        turned_real = real * cosine + imag * sine
        turned_imag = (imag * cosine - real * sine) * sign.astype(F32)
        along_u = spread(weights(pos_u), row_axis - lax.shift_right_logical(pos_u, 3))
        corner = r.col_s[s] & (SUB - 1)
        corner = jnp.where(mirror == 1, 1 - corner, corner) & (SUB - 1)
        start = (31 * mirror - sign * corner) - lax.shift_right_logical(pos_v, 3)
        along_v = spread(weights(pos_v), (col_axis + start) & (SUB - 1))
        left_h, left_l = two_parts(
            jnp.concatenate([along_u * turned_real, along_u * turned_imag], axis=0)
        )
        right_h, right_l = two_parts(along_v)
        block = dot(left_h, right_h, NT) + dot(left_l, right_h, NT) + dot(left_h, right_l, NT)
        odd = ((shifted + r.group_s[s]) & 1) == 1
        even_rows, odd_rows = [], []
        for ri in range(2):
            near, far = block[ri * 32 : ri * 32 + 16], block[ri * 32 + 16 : ri * 32 + 32]
            even_rows.append(jnp.where(odd, far, near))
            odd_rows.append(jnp.where(odd, near, far))
        return even_rows, odd_rows

    def pair(s, carry):
        here, there = one(s), one(s + SD // 2)
        for e in range(2):
            rows_ref[pl.ds(e * 256 + s, NC, stride=SD // 2), :] = jnp.concatenate(
                here[e] + there[e], axis=1
            )
        return carry

    lax.fori_loop(0, SD // 2, pair, 0, unroll=2)
    l0 = r.tile_v[...] * (G // NC) + r.col_v[...]
    l0 = jnp.where(mirror == 1, G - SUB + 1 - l0, l0).astype(F32)
    group = jnp.where(mirror == 1, 14 - r.group_v[...], r.group_v[...]).astype(F32)
    meta = jnp.concatenate(
        [jnp.concatenate([l0] * 4, axis=1), jnp.concatenate([group] * 4, axis=1)], axis=0
    )
    lane = lax.broadcasted_iota(jnp.int32, (2, 128), 1)
    mine = lax.shift_right_logical(lane, 5) == lax.rem(lax.axis_index("col"), 4)
    meta = jnp.where(mine, meta, 0.0)
    for k in range(2 * NC):
        out_ref[k, 0:16, :] = rows_ref[k * 16 : (k + 1) * 16, :]
        out_ref[k, 16:18, :] = meta


def unpack(r, z):
    recv_ref, u_h, u_l = r.recv_one, r.u_h, r.u_l
    lane = lax.broadcasted_iota(jnp.int32, (SD, 128), 1)
    sub = lax.broadcasted_iota(jnp.int32, (SD, 128), 0)
    segment = lax.shift_right_logical(lane[0:16], 5)
    data = recv_ref[z, 0:16, :]
    corner = recv_ref[z, 16:17, :]
    mine = lane == sub + SD * (z & 3)
    l0 = jnp.sum(
        jnp.where(mine, jnp.broadcast_to(corner, (SD, 128)), 0.0), axis=1, keepdims=True
    )
    distance = lane - (l0.astype(jnp.int32) & 127)
    rolled = [data] + [pltpu.roll(data, SUB * k, 1) for k in range(1, 4)]
    wide = []
    for i in range(4):
        v = rolled[(0 - i) % 4]
        for p in range(1, 4):
            v = jnp.where(segment == p, rolled[(p - i) % 4], v)
        wide.append(v)
    real = jnp.concatenate([wide[0], wide[2]], axis=0)
    imag = jnp.concatenate([wide[1], wide[3]], axis=0)
    in_a = (distance >= 0) & (distance < SUB)
    in_b = distance < SUB - 128
    for ab, inside in enumerate((in_a, in_b)):
        high, low = two_parts(
            jnp.concatenate(
                [jnp.where(inside, real, 0.0), jnp.where(inside, imag, 0.0)], axis=1
            )
        )
        at = pl.ds(pl.multiple_of(ab * 1024 + z * SD, SD), SD)
        u_h[at, :] = high
        u_l[at, :] = low


def exchange_one(r, row, col, half, opposite):
    send_ref, recv_ref = r.send_one, r.recv_one

    def copy(far, d):
        to = lax.rem(col + d, NC)
        there = half + far * (1 - 2 * half)
        return pltpu.make_async_remote_copy(
            src_ref=send_ref.at[there * NC + to],
            dst_ref=recv_ref.at[half * NC + col],
            send_sem=r.send_sem_one.at[0],
            recv_sem=r.recv_sem_one.at[far, d],
            device_id=(row + far * (opposite - row), to),
            device_id_type=MESH,
        )

    for far, d in ORDER_ONE:
        copy(far, d).start()
    own = pltpu.make_async_copy(
        send_ref.at[half * NC + col], recv_ref.at[half * NC + col], r.own_sem.at[0]
    )
    own.start()
    own.wait()
    unpack(r, half * NC + col)

    def arrive(i, carry):
        step = i // 2
        far = 1 - lax.rem(i, 2)
        d = 8 + ((step + 1) // 2) * (1 - 2 * lax.rem(step, 2))
        copy(far, d).wait_recv()
        there = half + far * (1 - 2 * half)
        unpack(r, there * NC + lax.rem(col + NC - d, NC))
        return carry

    lax.fori_loop(0, 2 * NC - 1, arrive, 0)


def rows(r, row, col):
    recv_ref, first_ref, turn_ref = r.recv_one, r.first, r.turn
    second_h, second_l, out_ref, extra_ref = r.second_h, r.second_l, r.send_two, r.extra
    u_h, u_l, a_h, a_l = r.u_h, r.u_l, r.a_h, r.a_l
    parity = row // HB
    shifted = jnp.where(col == 0, 1, 0)
    index = []
    for group in range(8):
        corner = sum(recv_ref[group * 4 + i, 16:17, :] for i in range(4)).astype(jnp.int32)
        start = sum(recv_ref[group * 4 + i, 17:18, :] for i in range(4)).astype(jnp.int32)
        if group >= 4:
            start = start + shifted
        start = lax.shift_right_logical(start + ((start ^ parity) & 1), 1) * 64
        tile = lax.shift_right_logical(corner, 7)
        index.append((start + tile, start + ((tile + 1) & 63)))
    chunks = [
        jnp.concatenate([index[k][ab], index[k + 1][ab]], axis=1)
        for ab in range(2)
        for k in range(0, 8, 2)
    ]

    def placed(first, count):
        place = lax.broadcasted_iota(jnp.int32, (count, 256), 0) + first
        total = jnp.zeros((count, 256), F32)
        for k in range(8):
            pick = (place == chunks[k]).astype(F32).astype(BF)
            at = slice(k * 256, (k + 1) * 256)
            total = total + dot(pick, u_h[at, :]) + dot(pick, u_l[at, :])
        return total

    def inner(value):
        high, low = two_parts(value)
        both = dot(first_ref[...], jnp.concatenate([high, high, low], axis=0))
        real = both[:64, :128] - both[64:, 128:]
        imag = both[64:, :128] + both[:64, 128:]
        cos, sin = turn_ref[0], turn_ref[1]
        return two_parts(
            jnp.concatenate([real * cos - imag * sin, real * sin + imag * cos], axis=1)
        )

    def outer(high, low):
        return (
            dot(second_h[...], high, NT) + dot(second_l[...], high, NT) + dot(second_h[...], low, NT)
        )

    def four_rows(block, carry):
        total = placed(block * 256, 256)
        for k in range(4):
            high, low = inner(total[k * 64 : (k + 1) * 64])
            for cl in range(4):
                at = pl.ds(pl.multiple_of(cl * 128 + (block * 4 + k) * 16, 16), 16)
                a_h[at, :] = high[cl * 16 : (cl + 1) * 16]
                a_l[at, :] = low[cl * 16 : (cl + 1) * 16]
        return carry

    lax.fori_loop(0, 2, four_rows, 0)
    for pair in range(2):
        at = slice(pair * 256, (pair + 1) * 256)
        done = outer(a_h[at, :], a_l[at, :])
        for ch in range(4):
            for k in range(2):
                at = slice(ch * 32, (ch + 1) * 32)
                real = done[:128][at, k * 128 : (k + 1) * 128]
                imag = done[128:][at, k * 128 : (k + 1) * 128]
                upper = (lax.broadcasted_iota(jnp.int32, (NR, 128), 1) & 8) != 0
                to = 4 * ch + 2 * pair + k
                out_ref[0, to] = jnp.where(upper, pltpu.roll(imag, 8, 1), real)
                out_ref[1, to] = jnp.where(upper, imag, pltpu.roll(real, 120, 1))

    def past_end():
        high, low = inner(placed(512, 64))
        done = outer(high, low)
        done = jnp.concatenate([done, jnp.zeros((256, 64), F32)], axis=1)
        where = lax.broadcasted_iota(jnp.int32, (8, 128), 1)
        where = lax.shift_right_logical(where, 4)
        for ch in range(4):
            for cl in range(4):
                v = jnp.zeros((8, 128), F32)
                for ri in range(2):
                    for part in range(4):
                        r0 = ri * 128 + ch * 32 + part * 8
                        to = part * 2 + ri
                        moved = pltpu.roll(done[r0 : r0 + 8], ((to - cl) * 16) % 128, 1)
                        v = jnp.where(where == to, moved, v)
                extra_ref[4 * ch + cl] = v

    return past_end


def swapped(x):
    upper = (lax.broadcasted_iota(jnp.int32, x.shape, 1) & 8) != 0
    return jnp.where(upper, pltpu.roll(x, 8, 1), pltpu.roll(x, 120, 1))


def joined(both):
    upper = (lax.broadcasted_iota(jnp.int32, (NR, 128), 1) & 8) != 0
    turned = swapped(both[NR:])
    return both[:NR] + jnp.where(upper, turned, -turned)


def later_stages(r, row, col, past_end, flat, up, down):
    send_ref, mid_ref, in_ref = r.send_two, r.mid, r.recv_two
    extra_ref, relay_ref, all_ref = r.extra, r.relay, r.extras
    sets = [lax.rem(col // PER + k, SETS) for k in (0, 1, 3, 2)]

    def first(part, d):
        to = lax.rem(col + d, NC)
        return pltpu.make_async_remote_copy(
            src_ref=send_ref.at[part, to],
            dst_ref=mid_ref.at[part, col],
            send_sem=r.send_a.at[0],
            recv_sem=r.recv_a.at[part * SETS + col // PER],
            device_id=(row, to),
            device_id_type=MESH,
        )

    def extra(to):
        return pltpu.make_async_remote_copy(
            src_ref=extra_ref.at[to],
            dst_ref=relay_ref,
            send_sem=r.send_x.at[0],
            recv_sem=r.recv_x.at[0],
            device_id=(row, to),
            device_id_type=MESH,
        )

    def spread_extra(e):
        return pltpu.make_async_remote_copy(
            src_ref=relay_ref,
            dst_ref=all_ref.at[row],
            send_sem=r.send_y.at[0],
            recv_sem=r.recv_y.at[0],
            device_id=(lax.rem(row + e, NR), col),
            device_id_type=MESH,
        )

    def second(part, g, e):
        to = lax.rem(row + e, NR)
        return pltpu.make_async_remote_copy(
            src_ref=mid_ref.at[part, pl.ds(g * PER, PER), pl.ds(to, 1)],
            dst_ref=in_ref.at[part, pl.ds(g * PER, PER), pl.ds(row, 1)],
            send_sem=r.send_b.at[0],
            recv_sem=r.recv_b.at[part * SETS + g],
            device_id=(to, col),
            device_id_type=MESH,
        )

    def relay(part, i):
        g = sets[i]
        block = pl.ds(g * PER, PER)
        landed(mid_ref.at[part, block], send_ref.at[part, block], r.recv_a.at[part * SETS + g])
        pltpu.make_async_copy(
            mid_ref.at[part, block, pl.ds(row, 1)],
            in_ref.at[part, block, pl.ds(row, 1)],
            r.recv_b.at[part * SETS + g],
        ).start()

        def go(e, carry):
            second(part, g, e).start()
            return carry

        lax.fori_loop(1, NR, go, 0)

    @pl.when(col == 0)
    def _():
        past_end()
        for d in range(1, NC):
            extra(d).start()
        pltpu.make_async_copy(extra_ref.at[0], relay_ref, r.recv_x.at[0]).start()

    for part in range(2):
        for d in ORDER_TWO:
            first(part, d).start()
        pltpu.make_async_copy(
            send_ref.at[part, col],
            mid_ref.at[part, col],
            r.recv_a.at[part * SETS + col // PER],
        ).start()

    relay(0, 0)
    relay(0, 1)
    landed(relay_ref, extra_ref.at[0], r.recv_x.at[0])
    pltpu.make_async_copy(relay_ref, all_ref.at[row], r.recv_y.at[0]).start()

    def go_extra(e, carry):
        spread_extra(e).start()
        return carry

    lax.fori_loop(1, NR, go_extra, 0)
    relay(0, 2)
    relay(0, 3)
    bands(r)
    relay(1, 0)
    first_digit(r, row, sets, 0, (0, 1))
    relay(1, 1)
    first_digit(r, row, sets, 0, (2, 3))
    relay(1, 2)
    other_digits(r, 0)
    last_digit(r, 0, up, down)
    relay(1, 3)
    first_digit(r, row, sets, 1, (0, 1, 2, 3))
    other_digits(r, 1)
    last_digit(r, 1, up, down)
    smooth(r, flat)


def finish(r, col):
    send_ref, mid_ref, across = r.send_two, r.mid, r.across
    most = pl.ds(0, 2 * NC - 1)
    landed(r.recv_one.at[most], r.send_one.at[most], r.send_sem_one.at[0])
    most = pl.ds(0, NC - 1)
    landed(mid_ref.at[:, most], send_ref.at[:, most], r.send_a.at[0])

    @pl.when(col == 0)
    def _():
        landed(r.extra.at[most], r.extra.at[most], r.send_x.at[0])

    most = pl.ds(0, NR - 1)
    landed(r.extras.at[most], r.extras.at[most], r.send_y.at[0])
    landed(mid_ref.at[:, :, most], send_ref.at[:, :, most], r.send_b.at[0])
    landed(across.at[:, 0:G], across.at[:, 0:G], r.send_h.at[0])


def first_digit(r, row, sets, part, steps):
    in_ref, first_ref, turn_one = r.recv_two, r.col_first, r.turn_one
    if part == 0 and 0 in steps:
        landed(r.extras, r.extras, r.recv_y.at[0])
    lane = lax.broadcasted_iota(jnp.int32, (HB, 128), 1)
    held = r.extras[0:HB, lax.rem(row, 8), :]
    mine = held
    for k in range(1, 4):
        mine = jnp.where(row // 8 == k, pltpu.roll(held, 128 - 32 * k, 1), mine)
    near = mine if part == 0 else pltpu.roll(mine, 120, 1)
    far = pltpu.roll(mine, 120 - 8 * part, 1)
    high, low = two_parts(jnp.where(lane < 8, near, jnp.where(lane < 16, far, 0.0)))
    added = joined(dot(first_ref[2], jnp.concatenate([high, high, low], axis=0)))

    def two(pair):
        for e in range(2):
            value = jnp.concatenate(
                [in_ref[part, pair * 2 + k, e * HB : (e + 1) * HB, :] for k in range(2)], axis=1
            )
            high, low = two_parts(value)
            done = dot(first_ref[e], jnp.concatenate([high, high, low], axis=0))
            for k in range(2):
                value = joined(done[:, k * 128 : (k + 1) * 128])
                if e == 0 and k == 0:
                    value = value + jnp.where(pair == 0, added, 0.0)
                high, low = two_parts(value * turn_one[0] + swapped(value) * turn_one[1])
                at = pl.ds(pl.multiple_of(e * 512 + (pair * 2 + k) * NR, NR), NR)
                r.y_h[at, :] = high
                r.y_l[at, :] = low

    for i in steps:
        g = sets[i]
        block = pl.ds(g * PER, PER)
        landed(in_ref.at[part, block], r.mid.at[part, block], r.recv_b.at[part * SETS + g])

        for k in range(PER // 2):
            two(g * (PER // 2) + k)


def other_digits(r, part):
    second_h, second_l, turn_two, middle = r.mix_h, r.mix_l, r.turn_two, r.middle

    def digits(n, carry):
        at = pl.ds(pl.multiple_of(n * 256, 256), 256)
        middle[:, at] = (
            dot(second_h[...], r.y_h[at, :], NT)
            + dot(second_l[...], r.y_h[at, :], NT)
            + dot(second_h[...], r.y_l[at, :], NT)
        )
        return carry

    lax.fori_loop(0, 4, digits, 0)

    def butterfly(k, carry):
        at = pl.ds(pl.multiple_of(k * 16, 16), 16)
        below = pl.ds(pl.multiple_of(64 + k * 16, 16), 16)

        def factor(n):
            return jnp.concatenate(
                [
                    jnp.broadcast_to(turn_two[n, pl.ds(2 * k + j, 1), :], (8, 512))
                    for j in range(2)
                ],
                axis=0,
            )

        real, imag = middle[at, 0:512], middle[below, 0:512]
        other_real, other_imag = middle[at, 512:1024], middle[below, 512:1024]
        cos, sin = factor(0), factor(1)
        other_real, other_imag = (
            other_real * cos - other_imag * sin,
            other_real * sin + other_imag * cos,
        )
        for half in range(2):
            if half == 0:
                one, two = real + other_real, imag + other_imag
            else:
                one, two = real - other_real, imag - other_imag
            cos, sin = factor(2 + 2 * half), factor(3 + 2 * half)
            high, low = two_parts(
                jnp.concatenate([one * cos - two * sin, one * sin + two * cos], axis=1)
            )
            to = pl.ds(pl.multiple_of(half * 64 + k * 16, 16), 16)
            r.z_h[to, :] = high
            r.z_l[to, :] = low
        return carry

    lax.fori_loop(0, 4, butterfly, 0)


def last_digit(r, part, up, down):
    image, third_h, third_l, z_h, z_l, own_ref = r.image, r.third_h, r.third_l, r.z_h, r.z_l, r.own
    rows = pl.ds(part * 8, 8)

    def sides(at, sem):
        return [
            pltpu.make_async_remote_copy(
                own_ref.at[rows, at],
                there.at[rows, at],
                r.send_h.at[0],
                r.recv_h.at[sem],
                device_id=peer,
                device_id_type=MESH,
            )
            for there, peer in ((r.low, up), (r.high, down))
        ]

    for half in range(2):
        at = slice(half * 256, (half + 1) * 256)
        image[:, at] = (
            dot(z_h[...], third_h[:, at])
            + dot(z_h[...], third_l[:, at])
            + dot(z_l[...], third_h[:, at])
        )
        for p2 in range(half * 8, half * 8 + 8):
            for group in range(4):
                own_ref[rows, p2 * 512 + group * 128 : p2 * 512 + (group + 1) * 128] = (
                    jnp.concatenate(
                        [
                            image[
                                (group * 4 + k) * 8 : (group * 4 + k + 1) * 8,
                                p2 * 32 : (p2 + 1) * 32,
                            ]
                            for k in range(4)
                        ],
                        axis=1,
                    )
                )
            if part == 1 and p2 % 4 == 3:
                for copy in sides(pl.ds(p2 // 4 * CHUNK, CHUNK), 1 + p2 // 4):
                    copy.start()
    if part == 0:
        for copy in sides(pl.ds(0, G), 0):
            copy.start()


def bands(r):
    taps_ref, across, band_h, band_l = r.taps, r.across, r.band_h, r.band_l
    mix = []
    for m in range(NSCALE):
        distance = lax.broadcasted_iota(jnp.int32, (16, 48), 1) - lax.broadcasted_iota(
            jnp.int32, (16, 48), 0
        )
        v = jnp.zeros((16, 48), F32)
        for t in range(KW):
            v = jnp.where(distance == t, taps_ref[m, t], v)
        mix.append(v)
    mix_h, mix_l = two_parts(jnp.concatenate(mix, axis=0))
    r.cross_mix[...] = jnp.concatenate([mix_h, mix_l, mix_h], axis=1)
    zero = jnp.zeros((NSCALE * 16, 128), F32)
    across[:, 0:128] = zero
    across[:, 128 + G : 256 + G] = zero
    band_h[...] = jnp.zeros_like(band_h)
    band_l[...] = jnp.zeros_like(band_l)
    difference = lax.broadcasted_iota(jnp.int32, (128, 128), 0) - lax.broadcasted_iota(
        jnp.int32, (128, 128), 1
    )
    for m in range(NSCALE):
        for k in range(3):
            distance = difference + (128 * k - 112)
            v = jnp.zeros((128, 128), F32)
            for t in range(KW):
                v = jnp.where(distance == t, taps_ref[m, t], v)
            high, low = two_parts(v)
            for o in range(2):
                at = slice((k + o) * 128, (k + o + 1) * 128)
                band_h[m, at, o * 128 : (o + 1) * 128] = high
                band_l[m, at, o * 128 : (o + 1) * 128] = low


def smooth(r, flat):
    own_ref, low_ref, high_ref = r.own, r.low, r.high
    across, band_h, band_l, result = r.across, r.band_h, r.band_l, r.out
    no_low, no_high = flat == 0, flat == NR * NC - 1

    def cross(i):
        here = slice(i * 512, (i + 1) * 512)
        below = jnp.where(no_low, 0.0, low_ref[:, here])
        above = jnp.where(no_high, 0.0, high_ref[:, here])
        high, low = two_parts(jnp.concatenate([below, own_ref[:, here], above], axis=0))
        across[:, i * 512 + 128 : i * 512 + 640] = dot(
            r.cross_mix[...], jnp.concatenate([high, high, low], axis=0)
        )

    def along(i):
        for m in range(NSCALE):
            window = jnp.concatenate(
                [
                    across[m * 16 : (m + 1) * 16, i * CHUNK + k * 256 : i * CHUNK + k * 256 + 512]
                    for k in range(8)
                ],
                axis=0,
            )
            high, low = two_parts(window)
            done = dot(high, band_h[m]) + dot(low, band_h[m]) + dot(high, band_l[m])
            for k in range(8):
                result[m, :, i * CHUNK + k * 256 : i * CHUNK + (k + 1) * 256] = done[
                    k * 16 : (k + 1) * 16
                ]

    landed(across.at[0:16, 0:G], across.at[0:16, 0:G], r.recv_h.at[0])
    for chunk in range(4):
        landed(across.at[0:16, 0:CHUNK], across.at[0:16, 0:CHUNK], r.recv_h.at[1 + chunk])
        for i in range(4):
            cross(chunk * 4 + i)
        if chunk:
            along(chunk - 1)
    along(3)


PRE = "hbm_"
GIVEN = "vis pos w".split() + "tile_v group_v col_v".split()
TABLES = (
    "first turn second_h second_l".split()
    + "col_first turn_one mix_h mix_l".split()
    + "turn_two third_h third_l".split()
)


def per_device(
    vis, vis_pos, vis_w, subgrid_tile, subgrid_group, subgrid_col, grid_kernel, scale_kernels
):
    tile, group = subgrid_tile[:, 0], subgrid_group[:, 0]
    tables = list(row_tables()) + list(column_tables())
    inputs = dict(
        group_s=(SM, group),
        col_s=(SM, subgrid_col),
        grid_taps=(SM, grid_kernel),
        taps=(SM, scale_kernels),
        hbm_vis=(ANY, vis),
        hbm_pos=(ANY, vis_pos),
        hbm_w=(ANY, vis_w.reshape(1, -1)),
        hbm_tile_v=(ANY, tile.reshape(1, -1)),
        hbm_group_v=(ANY, group.reshape(1, -1)),
        hbm_col_v=(ANY, subgrid_col.reshape(1, -1)),
    )
    for name, table in zip(TABLES, tables):
        inputs[PRE + name] = (ANY, jnp.asarray(table))
    dma = pltpu.SemaphoreType.DMA
    scratch = {name: pltpu.VMEM(t.shape, t.dtype) for name, t in zip(TABLES, tables)}
    scratch |= {
        n: pltpu.VMEM(inputs[PRE + n][1].shape, inputs[PRE + n][1].dtype) for n in GIVEN
    }
    scratch |= dict(
        given_sem=dma((len(GIVEN),)),
        table_sem=dma((len(TABLES),)),
        rows=pltpu.VMEM((512, 128), F32),
        send_one=pltpu.VMEM((2 * NC, MSG, 128), F32),
        recv_one=pltpu.VMEM((2 * NC, MSG, 128), F32),
        send_sem_one=dma((1,)),
        recv_sem_one=dma((2, NC)),
        own_sem=dma((1,)),
        u_h=pltpu.VMEM((2048, 256), BF),
        u_l=pltpu.VMEM((2048, 256), BF),
        a_h=pltpu.VMEM((512, 256), BF),
        a_l=pltpu.VMEM((512, 256), BF),
        send_two=pltpu.VMEM((2, NC, NR, 128), F32),
        extra=pltpu.VMEM((NC, 8, 128), F32),
        mid=pltpu.VMEM((2, NC, NR, 128), F32),
        relay=pltpu.VMEM((8, 128), F32),
        recv_two=pltpu.VMEM((2, NC, NR, 128), F32),
        extras=pltpu.VMEM((NR, 8, 128), F32),
        send_a=dma((1,)),
        recv_a=dma((2 * SETS,)),
        send_x=dma((1,)),
        recv_x=dma((1,)),
        send_y=dma((1,)),
        recv_y=dma((1,)),
        send_b=dma((1,)),
        recv_b=dma((2 * SETS,)),
        y_h=pltpu.VMEM((1024, 128), BF),
        y_l=pltpu.VMEM((1024, 128), BF),
        middle=pltpu.VMEM((128, 1024), F32),
        z_h=pltpu.VMEM((128, 1024), BF),
        z_l=pltpu.VMEM((128, 1024), BF),
        image=pltpu.VMEM((128, 512), F32),
        cross_mix=pltpu.VMEM((NSCALE * 16, 144), BF),
        own=pltpu.VMEM((16, G), F32),
        low=pltpu.VMEM((16, G), F32),
        high=pltpu.VMEM((16, G), F32),
        send_h=dma((1,)),
        recv_h=dma((5,)),
        across=pltpu.VMEM((NSCALE * 16, G + 256), F32),
        band_h=pltpu.VMEM((NSCALE, 512, 256), BF),
        band_l=pltpu.VMEM((NSCALE, 512, 256), BF),
    )
    names = list(inputs) + ["out"] + list(scratch)
    return pl.pallas_call(
        functools.partial(whole_kernel, names),
        out_shape=pltpu.VMEM((NSCALE, 16, G), F32),
        in_specs=[spec for spec, _ in inputs.values()],
        out_specs=VM,
        scratch_shapes=list(scratch.values()),
        compiler_params=pltpu.CompilerParams(collective_id=0, has_side_effects=True),
        name="whole",
    )(*[value for _, value in inputs.values()])


def solution(mesh):
    return jax.shard_map(
        per_device,
        mesh=mesh,
        in_specs=(
            P(None, ("row", "col")),
            P(None, ("row", "col")),
            P(("row", "col")),
            P(("row", "col"), None),
            P(("row", "col"), None),
            P(("row", "col")),
            P(),
            P(),
        ),
        out_specs=P(None, ("row", "col"), None),
        check_vma=False,
    )
```
